32 devices in a mesh: gx: 4 (over z), gy: 4 (over x, core), gz: 2 (over y).
Axes of the slice: x: 2, y: 2, z: 4, core: 2. Of those that a mesh axis runs over, the one named last changes fastest.
Arguments:
- krylov_basis: float32 [60, 16, 32, 256], P(None, 'gx', 'gy', 'gz'), may hold values from -6 to 6
- schur_vectors: float32 [60, 20], replicated, may hold values from -1 to 1, as said below
- next_vector: float32 [16, 32, 256], P('gx', 'gy', 'gz'), may hold values from -10 to 10
- diag_shift: float32 [16, 32, 256], P('gx', 'gy', 'gz'), may hold values from 0.25 to 2
- velocity: float32 [3, 16, 32, 256], P(None, 'gx', 'gy', 'gz'), may hold values from -1 to 1
Outputs:
- new_basis: float32 [24, 16, 32, 256], P(None, 'gx', 'gy', 'gz')
- hessenberg: float32 [24, 3], replicated
The draws below stay inside these ranges and needn't reach their ends.
Inputs may be any that keep to these rules, and one draw needn't show every extreme that they name: `schur_vectors`: the columns are orthonormal.
All inputs are finite; a program needn't handle non-finite values.
Results may differ from the reference program's by a relative error of at most 0.0003.
Values sent between devices are 32-bit elements; how exact they have to be, the bound alone decides.
A program may use at most 64 MiB of HBM per device.

```python
import jax
import jax.numpy as jnp
from jax import lax

BASIS = 60
KEEP = 20
EXPAND = 3
ROWS = 24
NX = 16
NY = 32
NZ = 256


def draw_schur_vectors(key, part):
    gaussian = jax.random.normal(key, (BASIS, KEEP), jnp.float32)
    orthonormal, triangle = jnp.linalg.qr(gaussian)
    return orthonormal.astype(jnp.float32)


def levels(stream_key, shape, split, least, largest):
    level = 1.0
    for axis_at, parts in split:
        heights = jax.random.uniform(jax.random.fold_in(jax.random.fold_in(stream_key, 6), axis_at), (parts,), jnp.float32, least / len(split), largest / len(split))
        level = level * jnp.repeat(jnp.exp(heights), shape[axis_at] // parts).reshape((-1,) + (1,) * (len(shape) - 1 - axis_at))
    return level


def noise(key, extent, scale, bound, shards=(), dtype=jnp.bfloat16):
    factor_of = levels(key, extent, shards, -0.22, 0.18) if shards else 1.0
    entries = jax.random.normal(key, extent, jnp.float32) * scale * factor_of
    return jnp.minimum(jnp.maximum(entries, -bound), bound).astype(dtype)


def setup_inputs(seed: int = 0) -> dict:
    key_list = jax.random.split(jax.random.key(seed), 6)
    krylov_basis = noise(key_list[0], (BASIS, NX, NY, NZ), 1.0, 6.0, ((1, 4), (2, 4), (3, 2)), jnp.float32)
    schur_vectors = draw_schur_vectors(jax.random.fold_in(key_list[5], 71), 0)
    next_vector = noise(key_list[2], (NX, NY, NZ), 2.0, 10.0, ((0, 4), (1, 4), (2, 2)), jnp.float32)
    diag_shift = jnp.clip(0.25 + 1.75 * jax.random.uniform(key_list[3], (NX, NY, NZ), jnp.float32) ** levels(key_list[3], (NX, NY, NZ), ((0, 4), (1, 4), (2, 2)), -0.2, 0.2), 0.25, 2.0)
    velocity = jnp.clip(jax.random.uniform(key_list[4], (3, NX, NY, NZ), jnp.float32, -1.0, 1.0) * levels(key_list[4], (3, NX, NY, NZ), ((1, 4), (2, 4), (3, 2)), -0.4, 0.0), -1.0, 1.0)
    return {"krylov_basis": krylov_basis, "schur_vectors": schur_vectors, "next_vector": next_vector, "diag_shift": diag_shift, "velocity": velocity}


def operate_field(field, diag_shift, velocity):
    padded = jnp.pad(field, 1)
    x_ahead = padded[2:, 1:-1, 1:-1]
    x_behind = padded[:-2, 1:-1, 1:-1]
    y_ahead = padded[1:-1, 2:, 1:-1]
    y_behind = padded[1:-1, :-2, 1:-1]
    z_ahead = padded[1:-1, 1:-1, 2:]
    z_behind = padded[1:-1, 1:-1, :-2]
    neighbours = x_ahead + x_behind + y_ahead + y_behind + z_ahead + z_behind
    flow = velocity[0] * (x_ahead - x_behind) + velocity[1] * (y_ahead - y_behind) + velocity[2] * (z_ahead - z_behind)
    return (6.0 + diag_shift) * field - neighbours + 0.5 * flow

def reference(krylov_basis, schur_vectors, next_vector, diag_shift, velocity):
    highest = lax.Precision.HIGHEST
    cell_count = NX * NY * NZ
    rotated = jnp.einsum('ik,ixyz->kxyz', schur_vectors, krylov_basis, precision=highest)
    norm_sq = jnp.sum(next_vector * next_vector) / cell_count
    first = next_vector / jnp.maximum(jnp.sqrt(norm_sq), 0.5)
    vectors = jnp.concatenate([rotated, first[None]], axis=0)
    columns = []
    for expansion in range(EXPAND):
        count = vectors.shape[0]
        flat_basis = vectors.reshape(count, -1)
        applied = operate_field(vectors[-1], diag_shift, velocity).reshape(-1)
        first_coeffs = jnp.dot(flat_basis, applied, precision=highest) / cell_count
        partly = applied - jnp.dot(first_coeffs, flat_basis, precision=highest)
        second_coeffs = jnp.dot(flat_basis, partly, precision=highest) / cell_count
        cleaned = partly - jnp.dot(second_coeffs, flat_basis, precision=highest)
        length = jnp.sqrt(jnp.sum(cleaned * cleaned) / cell_count)
        column = jnp.zeros((ROWS,), jnp.float32)
        column = column.at[:count].set(first_coeffs + second_coeffs).at[count].set(length)
        columns.append(column)
        newest = (cleaned / jnp.maximum(length, 0.5)).reshape(NX, NY, NZ)
        vectors = jnp.concatenate([vectors, newest[None]], axis=0)
    return (vectors, jnp.stack(columns, axis=1))
```

```python
import functools

import jax
import jax.numpy as jnp
from jax import lax
from jax.experimental import pallas as pl
from jax.experimental.pallas import tpu as pltpu
from jax.sharding import PartitionSpec as P

KEEP = 20
EXPAND = 3
ROWS = 24
LANES = 128
UNIT = 16
DIRECT = 64
AXES = ("gx", "gy", "gz")


def partner_steps(phase, sizes):
    xs = range(1, sizes[0]) if phase else ()
    steps = [(dx, 0, 0) for dx in xs] if phase == 1 else [
        (dx, dy, dz) for dx in tuple(reversed(xs)) + (0,)
        for dy in range(sizes[1]) for dz in range(sizes[2])]
    return [step for step in steps if step != (0, 0, 0)]


def body(
    sizes, cells,
    kry_hbm, schur_hbm, w_hbm, diag_hbm, vel_hbm,
    out, hess,
    schur, w_ref, diag, vel, kry, image, xr, yr, zr, ypack, zpack, xh, yh, zh, xs, ys, zs,
    gsend, grecv0, grecv1,
    rsend, rrecv0, rmid, rrecv1, msend, mrecv0, mmid, mrecv1, lsend, lrecv0, lmid, lrecv1,
    ubuf, abuf,
    load_sem, halo_send, halo_recv, gsem_s0, gsem_r0, gsem_s1, gsem_r1, sums_sem, ready,
):
    place = tuple(lax.axis_index(a) for a in AXES)
    basis = kry.shape[0]
    bx, by, bz = w_ref.shape
    loads = [
        pltpu.make_async_copy(source, target, load_sem.at[k])
        for k, (source, target) in enumerate((
            (w_hbm, w_ref), (schur_hbm, schur), (kry_hbm, kry), (diag_hbm, diag), (vel_hbm, vel)))
    ]
    for copy in loads:
        copy.start()
    direct = sizes[0] * sizes[1] * sizes[2] <= DIRECT
    shifted = [[lax.rem(place[d] + k, sizes[d]) for k in range(sizes[d])] for d in range(3)]

    def partners(phase):
        return [tuple(shifted[d][step[d]] for d in range(3))
                for step in partner_steps(phase, sizes)]


    for ref in (xr, yr, zr, xs, ys, zs):
        ref[...] = jnp.zeros_like(ref)

    barrier = pltpu.get_barrier_semaphore()
    for to in partners(0) + partners(1):
        pl.semaphore_signal(
            barrier, inc=1, device_id=to, device_id_type=pl.DeviceIdType.MESH)
    pl.semaphore_wait(barrier, len(partners(0)) + len(partners(1)))

    def halo_copies(kind, sources, targets):
        found = []
        for d in range(3):
            for side in (0, 1):
                at = (kind * 3 + d) * 2 + side
                to = list(place)
                to[d] = place[d] + (1 if side == 0 else -1)
                can_send = place[d] < sizes[d] - 1 if side == 0 else place[d] > 0
                can_recv = place[d] > 0 if side == 0 else place[d] < sizes[d] - 1
                found.append((
                    pltpu.make_async_remote_copy(
                        src_ref=sources[d][side], dst_ref=targets[d][side],
                        send_sem=halo_send.at[at], recv_sem=halo_recv.at[at],
                        device_id=tuple(to), device_id_type=pl.DeviceIdType.MESH,
                    ), can_send, can_recv))
        return found

    def halo_start(copies):
        for copy, can_send, _ in copies:
            pl.when(can_send)(copy.start)

    def halo_wait(copies):
        for copy, _, can_recv in copies:
            pl.when(can_recv)(copy.wait_recv)

    def halo_finish(copies):
        for copy, can_send, _ in copies:
            pl.when(can_send)(copy.wait_send)

    def field_copies(kind, ref):
        return halo_copies(
            kind,
            ((ref.at[bx - 1], ref.at[0]), (ref, ref), (ref, ref)),
            tuple((r.at[kind, 0], r.at[kind, 1]) for r in (xs, ys, zs)),
        )

    def exchange(send, slots, sem_s, sem_r, phase):
        for at, to in enumerate(partners(phase)):
            pltpu.make_async_remote_copy(
                src_ref=send, dst_ref=slots.at[at], send_sem=sem_s, recv_sem=sem_r,
                device_id=to, device_id_type=pl.DeviceIdType.MESH,
            ).start()
        pending.append(pltpu.make_async_copy(slots, slots, sem_s))
        return pltpu.make_async_copy(slots, slots, sem_r)

    def gather_sum(arrival, own, slots):
        arrival.wait()
        terms = [own] + [slots[k] for k in range(slots.shape[0])]
        while len(terms) > 1:
            terms = [sum(terms[k + 1:k + 2], terms[k]) for k in range(0, len(terms), 2)]
        return terms[0]

    pending = []

    def finish_sends():
        while pending:
            pending.pop().wait()

    groups = (
        (rsend, rrecv0, rmid, rrecv1), (msend, mrecv0, mmid, mrecv1), (lsend, lrecv0, lmid, lrecv1))

    def total_start(k, value):
        send, first = groups[k][:2]
        send[...] = value
        return exchange(send, first, sums_sem.at[k, 0], sums_sem.at[k, 1], 2 if direct else 0)

    def total_end(k, value, arrival):
        first, between, second = groups[k][1:]
        value = gather_sum(arrival, value, first)
        if not direct:
            between[...] = value
            arrival = exchange(between, second, sums_sem.at[k, 2], sums_sem.at[k, 3], 1)
            value = gather_sum(arrival, value, second)
        return value * (1.0 / cells)

    lane3 = lax.broadcasted_iota(jnp.int32, (by, bz), 1)
    row3 = lax.broadcasted_iota(jnp.int32, (by, bz), 0)

    def stencil(v, x_before, x_after, y_before, y_after, z_before, z_after):
        res = []
        for x in range(bx):
            here = v[x]
            xb = v[x - 1] if x > 0 else x_before
            xa = v[x + 1] if x < bx - 1 else x_after
            yb = jnp.where(row3 == 0, y_before[x], pltpu.roll(here, 1, 0))
            ya = jnp.where(row3 == by - 1, y_after[x], pltpu.roll(here, by - 1, 0))
            zb = jnp.where(lane3 == 0, z_before[x], pltpu.roll(here, 1, 1))
            za = jnp.where(lane3 == bz - 1, z_after[x], pltpu.roll(here, bz - 1, 1))
            neighbours = xa + xb + ya + yb + za + zb
            flow = (vel[0, x] * (xa - xb) + vel[1, x] * (ya - yb) + vel[2, x] * (za - zb))
            res.append((6.0 + diag[x]) * here - neighbours + 0.5 * flow)
        return res

    row8 = lax.broadcasted_iota(jnp.int32, (8, LANES), 0)

    def fold(tiles):
        for half in (4, 2, 1):
            low = (row8 & half) == 0
            tiles = [
                jnp.where(low, tiles[k] + pltpu.roll(tiles[k], 8 - half, 0),
                          tiles[k + half] + pltpu.roll(tiles[k + half], half, 0))
                for k in range(half)]
        return tiles[0]

    def dots(v, fields):
        groups = []
        for first in range(0, ROWS, 8):
            tiles = []
            for k in range(first, first + 8):
                field = fields[k] if k < len(fields) else None
                if field is None:
                    tiles.append(None)
                    continue
                total = field(0) * v[0]
                for x in range(1, bx):
                    total = total + field(x) * v[x]
                if by > 8:
                    total = sum(total[8 * t:8 * t + 8] for t in range(1, by // 8)) + total[0:8]
                tiles.append(total)
            if all(tile is None for tile in tiles):
                groups.append(jnp.zeros((8, bz), jnp.float32))
            else:
                groups.append(fold([
                    jnp.zeros((8, bz), jnp.float32) if t is None else t for t in tiles]))
        return jnp.sum(jnp.concatenate(groups, axis=0), axis=1, keepdims=True)

    def of(ref, *at):
        return lambda x: ref[at + (x,)]

    basis_fields = [of(out, i) for i in range(ROWS)]

    halo_w = field_copies(0, w_ref)
    loads[0].wait()
    halo_start(halo_w)
    if direct:
        for to in partners(1):
            pl.semaphore_signal(
                ready, inc=1, device_id=to, device_id_type=pl.DeviceIdType.MESH)

    out[KEEP + 1:ROWS] = jnp.zeros((ROWS - KEEP - 1, bx, by, bz), jnp.float32)
    out[KEEP] = w_ref[...]
    loads[1].wait()
    loads[2].wait()
    wide, deep = 5, 4
    for first in range(0, KEEP, wide):
        def step(at, sums, first=first):
            sums = list(sums)
            for k in range(deep):
                i = at * deep + k
                for x in range(bx):
                    tile = kry[i, x]
                    for j in range(wide):
                        sums[j * bx + x] = sums[j * bx + x] + schur[first + j, i] * tile
            return tuple(sums)
        sums = lax.fori_loop(
            0, basis // deep, step,
            tuple(jnp.zeros((by, bz), jnp.float32) for _ in range(wide * bx)))
        for j in range(wide):
            for x in range(bx):
                out[first + j, x] = sums[j * bx + x]

    for side, (near, edge) in enumerate(((by - 1, bz - 1), (0, 0))):
        for i in range(KEEP):
            ypack[side, i] = out[i, :, near, :]
        for x in range(bx):
            face = jnp.zeros((by, bz), jnp.float32)
            for i in range(KEEP):
                face = jnp.where(
                    lane3 == i, pltpu.roll(out[i, x], (i - edge) % bz, 1), face)
            zpack[side, x] = face
    halo_r = halo_copies(
        3,
        ((out.at[0:KEEP, bx - 1], out.at[0:KEEP, 0]), (ypack.at[0], ypack.at[1]),
         (zpack.at[0], zpack.at[1])),
        tuple((r.at[0], r.at[1]) for r in (xr, yr, zr)),
    )
    halo_start(halo_r)

    row = lax.broadcasted_iota(jnp.int32, (ROWS, LANES), 0)
    lane = lax.broadcasted_iota(jnp.int32, (ROWS, LANES), 1)
    lane1 = lax.broadcasted_iota(jnp.int32, (1, LANES), 1)
    row1 = lax.broadcasted_iota(jnp.int32, (ROWS, 1), 0)

    def as_row(col, shift=0):
        return jnp.sum(jnp.where(row + shift == lane, col, 0.0), axis=0, keepdims=True)

    def as_col(values):
        return jnp.sum(jnp.where(row == lane, values, 0.0), axis=1, keepdims=True)

    gram = jnp.zeros((ROWS, LANES), jnp.float32)
    for j in range(KEEP + 1):
        col = dots([out[j, x] for x in range(bx)],
                   [None] * (j // 8 * 8) + basis_fields[j // 8 * 8:KEEP + 1])
        gram = jnp.where((lane == j) & (row < KEEP + 1), col, gram)
    lane8 = lax.broadcasted_iota(jnp.int32, (8, LANES), 1)
    own8 = lane8 // UNIT == lax.broadcasted_iota(jnp.int32, (8, LANES), 0)

    def spread(value):
        for shift in (UNIT, 2 * UNIT, 4 * UNIT):
            value = value + pltpu.roll(value, shift, 1)
        return value

    units = (
        gram[16:24],
        gram[8:16],
        jnp.where(lane8 < 8, gram[0:8], pltpu.roll(gram[16:24], LANES - 8, 1)),
    )
    packed = jnp.concatenate([
        jnp.sum(jnp.where(own8, spread(jnp.where(lane8 < UNIT, unit, 0.0)), 0.0),
                axis=0, keepdims=True)
        for unit in units], axis=0)
    gsend[0] = packed
    if direct:
        pl.semaphore_wait(ready, sizes[0] - 1)
    arrival0 = exchange(gsend.at[0], grecv1, gsem_s1, gsem_r1, 2 if direct else 1)

    loads[3].wait()
    loads[4].wait()
    halo_wait(halo_w)
    applied = stencil(
        [w_ref[x] for x in range(bx)], xs[0, 0], xs[0, 1],
        [ys[0, 0, x, by - 1:by, :] for x in range(bx)],
        [ys[0, 1, x, 0:1, :] for x in range(bx)],
        [zs[0, 0, x, :, bz - 1:bz] for x in range(bx)],
        [zs[0, 1, x, :, 0:1] for x in range(bx)],
    )
    for x in range(bx):
        image[0, x] = applied[x]
    ownrow = as_row(dots(applied, basis_fields[:KEEP + 1] + [None, None, of(image, 0)]))
    row_arrival = total_start(0, ownrow)
    halo_a = field_copies(1, image.at[0])
    halo_start(halo_a)

    halo_wait(halo_r)
    for i in range(KEEP):
        found = stencil(
            [out[i, x] for x in range(bx)], xr[0, i], xr[1, i],
            [yr[0, i, x:x + 1] for x in range(bx)], [yr[1, i, x:x + 1] for x in range(bx)],
            [zr[0, x, :, i:i + 1] for x in range(bx)], [zr[1, x, :, i:i + 1] for x in range(bx)])
        for x in range(bx):
            ubuf[i, x] = found[x]
    ufields = [of(ubuf, i) for i in range(KEEP)]
    shares = [jnp.zeros((ROWS, LANES), jnp.float32) for _ in range(2)]
    for j in range(KEEP):
        v = [ubuf[j, x] for x in range(bx)]
        cols = (dots(v, basis_fields[:KEEP] + [of(w_ref), of(image, 0)]),
                dots(v, [None] * (j // 8 * 8) + ufields[j // 8 * 8:]))
        shares = [jnp.where(lane == j, col, part) for col, part in zip(cols, shares)]
    mixed = jnp.zeros((8, LANES), jnp.float32)
    for k in range(6):
        part = shares[k // 3][k % 3 * 8:k % 3 * 8 + 8]
        mixed = mixed + (part if k == 0 else pltpu.roll(part, KEEP * k, 1))
    mix_arrival = total_start(1, mixed)

    packed = gather_sum(arrival0, packed, grecv1)
    if not direct:
        gsend[1] = packed
        arrival1 = exchange(gsend.at[1], grecv0, gsem_s0, gsem_r0, 0)
        packed = gather_sum(arrival1, packed, grecv0)
    packed = packed * (1.0 / cells)
    units = [
        jnp.where(lane8 < UNIT,
                  spread(jnp.where(own8, jnp.broadcast_to(packed[u:u + 1], (8, LANES)), 0.0)),
                  0.0)
        for u in range(3)]
    corner = pltpu.roll(jnp.where(lane8 >= 8, units[2], 0.0), 8, 1)
    below = jnp.concatenate(
        [jnp.zeros((8, LANES), jnp.float32), jnp.where(lane8 < 8, units[1], 0.0), units[0],
         jnp.zeros((LANES - ROWS, LANES), jnp.float32)], axis=0)
    gram = jnp.concatenate(
        [jnp.where(lane8 < 8, units[2], 0.0), units[1], units[0] + corner], axis=0)
    gram = gram + below.T[0:ROWS]
    gram = jnp.where((lane < KEEP + 1) & (row < KEEP + 1), gram, 0.0)
    norm_sq = jnp.sum(
        jnp.sum(jnp.where((lane == KEEP) & (row == KEEP), gram, 0.0), axis=1, keepdims=True),
        axis=0, keepdims=True)
    scale = 1.0 / jnp.maximum(jnp.sqrt(norm_sq), 0.5)
    gram = gram * jnp.where(row == KEEP, scale, 1.0) * jnp.where(lane == KEEP, scale, 1.0)
    for x in range(bx):
        out[KEEP, x] = w_ref[x] * scale
    applied = [tile * scale for tile in applied]
    rowform = total_end(0, ownrow, row_arrival)
    rowform = rowform * scale * jnp.where((lane1 == KEEP) | (lane1 == ROWS - 1), scale, 1.0)

    for side in (0, 1):
        near_row, near_lane = (by - 1, bz - 1) if side == 0 else (0, 0)
        xh[side, 0] = xs[0, side] * scale
        for x in range(bx):
            yh[side, 0, x:x + 1] = ys[0, side, x, near_row:near_row + 1, :] * scale
            zh[side, x] = jnp.where(
                lane3 == KEEP, zs[0, side, x, :, near_lane:near_lane + 1] * scale, zr[side, x])
    for x in range(bx):
        abuf[x] = applied[x]
    hcols = []

    def step(count, c_row, c_col, image_sq, gram):
        twice = jnp.where(row == lane, 2.0, 0.0) - gram
        if c_col is None:
            t_col = jnp.sum(twice * c_row, axis=1, keepdims=True)
            t_row = as_row(t_col)
        else:
            t_row = jnp.sum(twice * c_col, axis=0, keepdims=True)
            t_col = as_col(t_row)
        weights = jnp.broadcast_to(t_col, (ROWS, LANES))
        gt_row = jnp.sum(gram * weights, axis=0, keepdims=True)
        length_sq = image_sq + jnp.sum(t_row * (gt_row - 2.0 * c_row), axis=1, keepdims=True)
        length_sq = jnp.maximum(length_sq, 0.0)
        length = jnp.sqrt(length_sq)
        inverse = 1.0 / jnp.maximum(length, 0.5)
        hcols.append(jnp.where(lane1 == count, length, t_row))
        return t_row, t_col, weights, length_sq, inverse

    def less(start, weights, fields):
        for i, field in enumerate(fields):
            weight = jnp.broadcast_to(weights[i:i + 1, :], (by, bz))
            start = [start[x] - weight * field(x) for x in range(bx)]
        return start

    def widen(gram, count, t_row, c_row, length_sq, inverse):
        e_row = t_row - c_row
        e_col = as_col(e_row)
        cross_col = (e_col - jnp.sum(gram * e_row, axis=1, keepdims=True)) * inverse
        cross_row = (e_row - jnp.sum(gram * e_col, axis=0, keepdims=True)) * inverse
        corner = length_sq * inverse * inverse
        gram = jnp.where(row == count, cross_row, jnp.where(lane == count, cross_col, gram))
        return jnp.where((row == count) & (lane == count), corner, gram)

    def pick(values, at):
        return jnp.sum(jnp.where(lane1 == at, values, 0.0), axis=1, keepdims=True)

    count = KEEP + 1
    first_row = jnp.where(lane1 < count, rowform, 0.0)
    image_sq = pick(rowform, ROWS - 1)
    t_row, t_col, weights, length_sq, inverse = step(count, first_row, None, image_sq, gram)
    newest = [tile * inverse for tile in less(applied, weights, basis_fields[:count])]
    for x in range(bx):
        out[count, x] = newest[x]
    halo_wait(halo_a)
    sides = []
    for side in (0, 1):
        near_row, near_lane = (by - 1, bz - 1) if side == 0 else (0, 0)
        x_part = xs[1, side] * scale
        y_part = [ys[1, side, x, near_row:near_row + 1, :] * scale for x in range(bx)]
        y_part = jnp.concatenate(y_part, axis=0)
        for i in range(count):
            weight = weights[i:i + 1, :]
            x_part = x_part - weight * (xr[side, i] if i < KEEP else xh[side, 0])
            y_part = y_part - weight * (yr[side, i] if i < KEEP else yh[side, 0])
        x_part = x_part * inverse
        y_part = y_part * inverse
        z_part = [
            (zs[1, side, x, :, near_lane:near_lane + 1] * scale
             - jnp.sum(zh[side, x] * t_row, axis=1, keepdims=True)) * inverse
            for x in range(bx)]
        sides.append((x_part, [y_part[x:x + 1] for x in range(bx)], z_part))
    second = stencil(newest, sides[0][0], sides[1][0], sides[0][1], sides[1][1],
                     sides[0][2], sides[1][2])
    for x in range(bx):
        image[1, x] = second[x]
    halo_p = field_copies(2, image.at[1])
    halo_start(halo_p)
    gram = widen(gram, count, t_row, first_row, length_sq, inverse)

    count = KEEP + 2
    grown = ufields + [of(abuf), of(image, 1)]
    p_row = (as_row(dots(second, basis_fields[:count]))
             + as_row(dots(second, grown), 32))
    q_row = as_row(dots(newest, grown[:KEEP + 1]), 32)
    halo_wait(halo_p)
    third = stencil(
        second, xs[2, 0], xs[2, 1],
        [ys[2, 0, x, by - 1:by, :] for x in range(bx)],
        [ys[2, 1, x, 0:1, :] for x in range(bx)],
        [zs[2, 0, x, :, bz - 1:bz] for x in range(bx)],
        [zs[2, 1, x, :, 0:1] for x in range(bx)],
    )
    r_row = (as_row(dots(third, basis_fields[:count]))
             + as_row(dots(third, grown + [lambda x: third[x]]), 32))
    last = jnp.concatenate([p_row, r_row, q_row], axis=0)
    earlier = pending[:]
    pending.clear()
    last_arrival = total_start(2, last)
    for copy in earlier:
        copy.wait()
    for copies in (halo_w, halo_r, halo_a, halo_p):
        halo_finish(copies)
    mixed = total_end(1, mixed, mix_arrival)
    parts = [jnp.where(lane8 < KEEP,
                       mixed if k == 0 else pltpu.roll(mixed, LANES - KEEP * k, 1), 0.0)
             for k in range(6)]
    across = jnp.concatenate(parts[0:3], axis=0)
    inside = jnp.concatenate(parts[3:6], axis=0)
    image_row = across[KEEP + 1:KEEP + 2] * scale
    across = jnp.where(row < KEEP, across, jnp.where(row == KEEP, across * scale, 0.0))
    across = jnp.where((lane == KEEP) & (row <= KEEP), as_col(first_row), across)
    inside = inside * jnp.where(row // 8 > lane // 8, 2.0, 1.0)
    inside = jnp.where(row == KEEP, jnp.where(lane == KEEP, image_sq, 2.0 * image_row), inside)

    last = total_end(2, last, last_arrival)
    shifted_last = pltpu.roll(last, LANES - 32, 1)
    c_row = jnp.where(lane1 < count, last[0:1], 0.0)
    pz_row = jnp.where(lane1 < count, shifted_last[0:1], 0.0)
    rq_row = jnp.where(lane1 < count, last[1:2], 0.0)
    rz_row = jnp.where(lane1 <= count, shifted_last[1:2], 0.0)
    qz_row = jnp.where(lane1 < KEEP + 1, shifted_last[2:3], 0.0)
    across = jnp.where(row == KEEP + 1, qz_row, across)
    across = jnp.where((lane == KEEP + 1) & (row < count), as_col(c_row), across)
    inside = jnp.where(row == KEEP + 1,
                       jnp.where(lane == KEEP + 1, pz_row, 2.0 * pz_row), inside)
    t_row, t_col, weights, length_sq, inverse = step(
        count, c_row, None, pick(pz_row, KEEP + 1), gram)
    gram = widen(gram, count, t_row, c_row, length_sq, inverse)
    h_col = jnp.sum(jnp.where(row == lane, rq_row, 0.0) - across * t_row, axis=1, keepdims=True)
    th = jnp.sum(t_col * h_col, axis=0, keepdims=True)
    corner = jnp.sum(jnp.where(lane1 == KEEP + 1, rz_row, 0.0) - pz_row * t_row,
                     axis=1, keepdims=True)
    corner = (corner - th) * inverse * inverse
    wt_row = jnp.sum(inside * t_col, axis=0, keepdims=True)
    image_sq = jnp.sum(
        jnp.where(lane1 == count, rz_row, (wt_row - 2.0 * rz_row) * t_row),
        axis=1, keepdims=True) * inverse * inverse
    c_col = jnp.where(row1 < count, h_col * inverse, jnp.where(row1 == count, corner, 0.0))
    newest = [tile * inverse for tile in less(second, weights, basis_fields[:count])]
    for x in range(bx):
        out[count, x] = newest[x]
    applied = [tile * inverse for tile in less(third, weights, grown)]
    count = KEEP + 3
    t_row, t_col, weights, length_sq, inverse = step(count, as_row(c_col), c_col, image_sq, gram)
    newest = [tile * inverse for tile in less(applied, weights, basis_fields[:count])]
    for x in range(bx):
        out[count, x] = newest[x]

    for k in range(EXPAND):
        hess[k:k + 1] = hcols[k]
    finish_sends()


def per_device(krylov_basis, schur_vectors, next_vector, diag_shift, velocity):
    sizes = tuple(lax.axis_size(a) for a in AXES)
    block = next_vector.shape
    bx, by, bz = block
    cells = float(bx * by * bz * sizes[0] * sizes[1] * sizes[2])
    n0, n1 = sizes[1] * sizes[2], sizes[0]
    nrow = n0 * n1 if n0 * n1 <= DIRECT else n0
    nline = n0 * n1 if n0 * n1 <= DIRECT else n1
    f32 = jnp.float32
    vmem = pl.BlockSpec(memory_space=pltpu.VMEM)
    dma = pltpu.SemaphoreType.DMA
    vectors, columns = pl.pallas_call(
        functools.partial(body, sizes, cells),
        out_shape=(
            pltpu.VMEM((ROWS,) + block, f32),
            pltpu.VMEM((8, LANES), f32),
        ),
        in_specs=[
            pl.BlockSpec(memory_space=pl.ANY) for _ in range(5)
        ],
        out_specs=(vmem, vmem),
        scratch_shapes=[
            pltpu.SMEM(schur_vectors.shape[::-1], f32),
            pltpu.VMEM(block, f32),
            pltpu.VMEM(block, f32),
            pltpu.VMEM((3,) + block, f32),
            pltpu.VMEM(krylov_basis.shape, f32),
            pltpu.VMEM((2,) + block, f32),
            pltpu.VMEM((2, KEEP, by, bz), f32),
            pltpu.VMEM((2, KEEP, bx, bz), f32),
            pltpu.VMEM((2,) + block, f32),
            pltpu.VMEM((2, KEEP, bx, bz), f32),
            pltpu.VMEM((2,) + block, f32),
            pltpu.VMEM((2, EXPAND, by, bz), f32),
            pltpu.VMEM((2, EXPAND, bx, bz), f32),
            pltpu.VMEM((2,) + block, f32),
            pltpu.VMEM((EXPAND, 2, by, bz), f32),
            pltpu.VMEM((EXPAND, 2) + block, f32),
            pltpu.VMEM((EXPAND, 2) + block, f32),
            pltpu.VMEM((2, 3, LANES), f32),
            pltpu.VMEM((n0 - 1, 3, LANES), f32),
            pltpu.VMEM((nline - 1, 3, LANES), f32),
            *[pltpu.VMEM(shape, f32) for rows in (1, 8, 3) for shape in (
                (rows, LANES), (nrow - 1, rows, LANES), (rows, LANES), (n1 - 1, rows, LANES))],
            pltpu.VMEM((KEEP,) + block, f32),
            pltpu.VMEM(block, f32),
            dma((5,)), dma((24,)), dma((24,)),
            dma, dma, dma, dma,
            dma((3, 4)),
            pltpu.SemaphoreType.REGULAR,
        ],
        compiler_params=pltpu.CompilerParams(collective_id=0, has_side_effects=True),
    )(krylov_basis, schur_vectors.T, next_vector, diag_shift, velocity)
    return vectors, columns[0:EXPAND, 0:ROWS].T


def solution(mesh):
    in_specs = (
        P(None, "gx", "gy", "gz"),
        P(),
        P("gx", "gy", "gz"),
        P("gx", "gy", "gz"),
        P(None, "gx", "gy", "gz"),
    )
    out_specs = (P(None, "gx", "gy", "gz"), P())
    return jax.shard_map(
        per_device, mesh=mesh, in_specs=in_specs, out_specs=out_specs, check_vma=False
    )
```

```python
import functools
import math

import jax
import jax.numpy as jnp
from jax import lax
from jax.experimental import pallas as pl
from jax.experimental.pallas import tpu as pltpu
from jax.sharding import PartitionSpec as P

KEEP = 20
EXPAND = 3
ROWS = 24
LANES = 128
DIRECT = 64
CHUNK = 5
MIX = 1
NEAR = 2
AXES = ("gx", "gy", "gz")


def turns_of(line):
    return -(-max(line - 2, 0) // NEAR) + 1 if line > 1 else 0


def partner_steps(phase, sizes):
    xs = range(1, sizes[0]) if phase else ()
    steps = [(dx, 0, 0) for dx in xs] if phase == 1 else [
        (dx, dy, dz) for dx in tuple(reversed(xs)) + (0,)
        for dy in range(sizes[1]) for dz in range(sizes[2])]
    return [step for step in steps if step != (0, 0, 0)]


def body(
    sizes, cells,
    kry_hbm, schur_hbm, w_hbm, diag_hbm, vel_hbm,
    out, hess,
    schur, w_ref, diag, vel, kry, image, xr, yr, zr, ypack, zpack, xh, yh, zh, yhpack, zhpack, xs, ys, zs,
    rsend, rrecv0, rmid, rrecv1, msend, mrecv0, mmid, mrecv1, lsend, lrecv0, lmid, lrecv1,
    ubuf, abuf, pbuf,
    load_sem, halo_send, halo_recv, sums_sem, line_sem, ready,
):
    place = tuple(lax.axis_index(a) for a in AXES)
    basis = kry_hbm.shape[0]
    bx, by, bz = w_ref.shape
    loads = [
        pltpu.make_async_copy(source, target, load_sem.at[k])
        for k, (source, target) in enumerate((
            (w_hbm, w_ref), (schur_hbm, schur), (kry_hbm, kry.at[0:basis]), (diag_hbm, diag),
            (vel_hbm, vel)))
    ]
    for copy in loads:
        copy.start()
    direct = sizes[0] * sizes[1] * sizes[2] <= DIRECT
    shifted = [[lax.rem(place[d] + k, sizes[d]) for k in range(sizes[d])] for d in range(3)]

    def partners(phase):
        return [tuple(shifted[d][step[d]] for d in range(3))
                for step in partner_steps(phase, sizes)]


    for ref in (xr, yr, zr, xh, yh, zh, xs, ys, zs):
        ref[...] = jnp.zeros_like(ref)

    barrier = pltpu.get_barrier_semaphore()
    line = [
        ((place[0] + step,) + place[1:],
         place[0] < sizes[0] - step if step > 0 else place[0] >= -step)
        for far in range(1, min(NEAR, sizes[0] - 1) + 1) for step in (far, -far)]

    def tell(semaphore, to):
        pl.semaphore_signal(
            semaphore, inc=1, device_id=to, device_id_type=pl.DeviceIdType.MESH)

    for to in partners(0) + ([] if direct else partners(1)):
        tell(barrier, to)
    if direct:
        for to, near in line:
            pl.when(near)(functools.partial(tell, barrier, to))
    turns_needed = turns_of(sizes[0]) if direct else 0

    def pass_on(turn):
        if 0 < turn <= turns_needed:
            for side, (to, near) in enumerate(line if turn < turns_needed else line[:2]):
                pl.when(near)(functools.partial(pl.semaphore_wait, ready.at[turn - 1, side], 1))
        if turn < turns_needed:
            for side, (to, near) in enumerate(line if turn + 1 < turns_needed else line[:2]):
                pl.when(near)(functools.partial(tell, ready.at[turn, side ^ 1], to))


    sent = [[] for _ in range(3)]

    def halo_start(kind, dims, sources, targets):
        for d in dims:
            for side in (0, 1):
                to = list(place)
                to[d] = place[d] + (1 if side == 0 else -1)
                can_send = place[d] < sizes[d] - 1 if side == 0 else place[d] > 0
                source = sources[d][side]
                sent[d].append(math.prod(source.shape))
                pl.when(can_send)(pltpu.make_async_remote_copy(
                    src_ref=source, dst_ref=targets[d][side],
                    send_sem=halo_send.at[d], recv_sem=halo_recv.at[kind, d],
                    device_id=tuple(to), device_id_type=pl.DeviceIdType.MESH).start)

    def landed(ref, semaphore):
        pltpu.make_async_copy(ref, ref, semaphore).wait()

    def halo_wait(kind, targets):
        for d in range(3):
            before, after = place[d] > 0, place[d] < sizes[d] - 1
            semaphore = halo_recv.at[kind, d]
            if sizes[d] > 2:
                pl.when(before & after)(functools.partial(landed, targets[d], semaphore))
                pl.when(before != after)(functools.partial(landed, targets[d].at[0], semaphore))
            elif sizes[d] == 2:
                landed(targets[d].at[0], semaphore)

    def halo_finish():
        for d in range(3):
            before, after = place[d] > 0, place[d] < sizes[d] - 1
            tiles = sum(sent[d]) // 2 // (by * bz)
            if sizes[d] > 2:
                pl.when(before & after)(functools.partial(
                    landed, kry.at[0:tiles, 0:2], halo_send.at[d]))
                pl.when(before != after)(functools.partial(
                    landed, kry.at[0:tiles, 0], halo_send.at[d]))
            elif sizes[d] == 2:
                landed(kry.at[0:tiles, 0], halo_send.at[d])

    def field_targets(kind):
        return tuple(r.at[kind] for r in (xs, ys, zs))

    def field_start(kind, ref):
        halo_start(kind, range(3), ((ref.at[bx - 1], ref.at[0]), (ref, ref), (ref, ref)),
                   tuple((r.at[0], r.at[1]) for r in field_targets(kind)))

    def exchange(send, slots, sem_s, sem_r, phase):
        for at, to in enumerate(partners(phase)):
            pltpu.make_async_remote_copy(
                src_ref=send, dst_ref=slots.at[at], send_sem=sem_s, recv_sem=sem_r,
                device_id=to, device_id_type=pl.DeviceIdType.MESH,
            ).start()
        pending.append(pltpu.make_async_copy(slots, slots, sem_s))
        return pltpu.make_async_copy(slots, slots, sem_r)

    def gather_sum(arrival, own, slots):
        arrival.wait()
        terms = [own] + [slots[k] for k in range(slots.shape[0])]
        while len(terms) > 1:
            terms = [sum(terms[k + 1:k + 2], terms[k]) for k in range(0, len(terms), 2)]
        return terms[0]

    pending = []

    def finish_sends():
        while pending:
            pending.pop().wait()

    groups = (
        (rsend, rrecv0, rmid, rrecv1), (msend, mrecv0, mmid, mrecv1), (lsend, lrecv0, lmid, lrecv1))

    def total_start(k, value):
        send, first = groups[k][:2]
        send[...] = value
        return exchange(send, first, sums_sem.at[2 * k], sums_sem.at[2 * k + 1],
                        2 if direct and k != MIX else 0)

    def total_end(k, value, arrival):
        first, between, second = groups[k][1:]
        value = gather_sum(arrival, value, first)
        if not direct or k == MIX:
            at = 0 if direct else k
            between[...] = value
            arrival = exchange(between, second, line_sem.at[2 * at], line_sem.at[2 * at + 1], 1)
            value = gather_sum(arrival, value, second)
        return value * (1.0 / cells)

    lane3 = lax.broadcasted_iota(jnp.int32, (by, bz), 1)
    row3 = lax.broadcasted_iota(jnp.int32, (by, bz), 0)

    def stencil(v, x_before, x_after, y_before, y_after, z_before, z_after):
        res = []
        for x in range(bx):
            here = v[x]
            xb = v[x - 1] if x > 0 else x_before
            xa = v[x + 1] if x < bx - 1 else x_after
            yb = jnp.where(row3 == 0, y_before[x], pltpu.roll(here, 1, 0))
            ya = jnp.where(row3 == by - 1, y_after[x], pltpu.roll(here, by - 1, 0))
            zb = jnp.where(lane3 == 0, z_before[x], pltpu.roll(here, 1, 1))
            za = jnp.where(lane3 == bz - 1, z_after[x], pltpu.roll(here, bz - 1, 1))
            neighbours = xa + xb + ya + yb + za + zb
            flow = (vel[0, x] * (xa - xb) + vel[1, x] * (ya - yb) + vel[2, x] * (za - zb))
            res.append((6.0 + diag[x]) * here - neighbours + 0.5 * flow)
        return res

    row8 = lax.broadcasted_iota(jnp.int32, (8, LANES), 0)

    def fold(tiles):
        for half in (4, 2, 1):
            low = (row8 & half) == 0
            tiles = [
                jnp.where(low, tiles[k] + pltpu.roll(tiles[k], 8 - half, 0),
                          tiles[k + half] + pltpu.roll(tiles[k + half], half, 0))
                for k in range(half)]
        return tiles[0]

    def dots(v, fields):
        groups = []
        for first in range(0, ROWS, 8):
            tiles = []
            for k in range(first, first + 8):
                field = fields[k] if k < len(fields) else None
                if field is None:
                    tiles.append(None)
                    continue
                total = field(0) * v[0]
                for x in range(1, bx):
                    total = total + field(x) * v[x]
                if by > 8:
                    total = sum(total[8 * t:8 * t + 8] for t in range(1, by // 8)) + total[0:8]
                tiles.append(total)
            if all(tile is None for tile in tiles):
                groups.append(jnp.zeros((8, bz), jnp.float32))
            else:
                groups.append(fold([
                    jnp.zeros((8, bz), jnp.float32) if t is None else t for t in tiles]))
        return jnp.sum(jnp.concatenate(groups, axis=0), axis=1, keepdims=True)

    def of(ref, *at):
        return lambda x: ref[at + (x,)]

    basis_fields = [of(out, i) for i in range(ROWS)]

    loads[0].wait()

    out[KEEP + 1:ROWS] = jnp.zeros((ROWS - KEEP - 1, bx, by, bz), jnp.float32)
    out[KEEP] = w_ref[...]
    deep = kry.shape[0]
    for i in range(basis, deep):
        kry[i] = jnp.zeros((bx, by, bz), jnp.float32)
    loads[1].wait()

    def halves(value):
        high = value.astype(jnp.bfloat16).astype(jnp.float32)
        return high, value - high

    def times(a, b):
        return lax.dot_general(a, b, (((1,), (0,)), ((), ())),
                               precision=lax.Precision.DEFAULT,
                               preferred_element_type=jnp.float32)

    spread = (lax.broadcasted_iota(jnp.int32, (basis, deep * by), 1) // by
              == lax.broadcasted_iota(jnp.int32, (basis, deep * by), 0)).astype(jnp.float32)
    same = (lax.broadcasted_iota(jnp.int32, (by, deep * by), 1) % by
            == lax.broadcasted_iota(jnp.int32, (by, deep * by), 0))
    turns = []
    for part in halves(schur[...]):
        wide = times(part, spread)
        turns.append(jnp.concatenate(
            [jnp.where(same, jnp.broadcast_to(wide[j:j + 1], same.shape), 0.0)
             for j in range(KEEP)], axis=0))
    both = jnp.concatenate(turns, axis=0)
    loads[2].wait()
    for x in range(0, bx, 2):
        pair = range(x, min(x + 2, bx))
        tiles = jnp.concatenate([kry[:, k].reshape(deep * by, bz) for k in pair], axis=1)
        high, low = halves(tiles)
        first = times(both, high)
        found = first[:KEEP * by] + (first[KEEP * by:] + times(turns[0], low))
        for j in range(KEEP):
            for k in pair:
                out[j, k] = found[j * by:(j + 1) * by, (k - x) * bz:(k - x + 1) * bz]

    pl.semaphore_wait(barrier, len(partners(0)) + (
        sum(near.astype(jnp.int32) for _, near in line) if direct else len(partners(1))))
    field_start(0, w_ref)
    pass_on(0)

    def face_start(kind, ref, packs, targets, dims, span):
        (ys_, zs_), (first, last) = packs, span
        halo_start(
            kind, dims,
            ((ref.at[first:last, bx - 1], ref.at[first:last, 0]), (ys_.at[0], ys_.at[1]),
             (zs_.at[0], zs_.at[1])),
            tuple((r.at[0, first:last], r.at[1, first:last]) if d == 0 else (r.at[0], r.at[1])
                  for d, r in enumerate(targets)))

    def pack_faces(ref, packs):
        ys_, zs_ = packs
        for side, (near, edge) in enumerate(((by - 1, bz - 1), (0, 0))):
            for i in range(KEEP):
                ys_[side, i] = ref[i, :, near, :]
            for x in range(bx):
                face = jnp.zeros((by, bz), jnp.float32)
                for i in range(KEEP):
                    face = jnp.where(
                        lane3 == i, pltpu.roll(ref[i, x], (i - edge) % bz, 1), face)
                zs_[side, x] = face

    turned = (3, out, (ypack, zpack), (xr, yr, zr))
    face_start(*turned, (0,), (0, KEEP))
    pack_faces(out, (ypack, zpack))
    face_start(*turned, (1, 2), (0, KEEP))
    pass_on(1)

    row = lax.broadcasted_iota(jnp.int32, (ROWS, LANES), 0)
    lane = lax.broadcasted_iota(jnp.int32, (ROWS, LANES), 1)
    lane1 = lax.broadcasted_iota(jnp.int32, (1, LANES), 1)
    row1 = lax.broadcasted_iota(jnp.int32, (ROWS, 1), 0)

    def as_row(col, shift=0):
        return jnp.sum(jnp.where(row + shift == lane, col, 0.0), axis=0, keepdims=True)

    def as_col(values):
        return jnp.sum(jnp.where(row == lane, values, 0.0), axis=1, keepdims=True)

    gram = jnp.zeros((ROWS, LANES), jnp.float32)
    for j in range(KEEP + 1):
        col = dots([out[j, x] for x in range(bx)],
                   [None] * (j // 8 * 8) + basis_fields[j // 8 * 8:KEEP + 1])
        gram = jnp.where((lane == j) & (row < KEEP + 1), col, gram)
    lane8 = lax.broadcasted_iota(jnp.int32, (8, LANES), 1)
    below = jnp.where(row // 8 > lane // 8, gram, 0.0)
    gram = gram + jnp.concatenate(
        [below, jnp.zeros((LANES - ROWS, LANES), jnp.float32)], axis=0).T[0:ROWS]

    loads[3].wait()
    loads[4].wait()
    halo_wait(0, field_targets(0))
    applied = stencil(
        [w_ref[x] for x in range(bx)], xs[0, 0], xs[0, 1],
        [ys[0, 0, x, by - 1:by, :] for x in range(bx)],
        [ys[0, 1, x, 0:1, :] for x in range(bx)],
        [zs[0, 0, x, :, bz - 1:bz] for x in range(bx)],
        [zs[0, 1, x, :, 0:1] for x in range(bx)],
    )
    for x in range(bx):
        image[0, x] = applied[x]
    field_start(1, image.at[0])
    own_sq = jnp.sum(jnp.where((row == KEEP) & (lane == KEEP), gram, 0.0),
                     axis=0, keepdims=True)
    own_sq = jnp.sum(own_sq, axis=1, keepdims=True)
    own = dots(applied, basis_fields[:KEEP + 1] + [None, None, of(image, 0)])
    own = jnp.where(row1 == KEEP + 1, own_sq, own)
    gram = jnp.where(lane < KEEP, gram, jnp.where(lane == KEEP, own, 0.0))
    cut = KEEP + 1
    packed = gram[0:8] + pltpu.roll(gram[8:16], cut, 1) + pltpu.roll(gram[16:24], 2 * cut, 1)
    packed = packed[0:4] + pltpu.roll(packed[4:8], 3 * cut, 1)
    for turn in range(2, turns_needed + 1):
        pass_on(turn)
    first_arrival = total_start(0, packed)

    halo_wait(3, (xr, yr, zr))
    applied_faces = (4, ubuf, (yhpack, zhpack), (xh, yh, zh))
    for i in range(KEEP):
        found = stencil(
            [out[i, x] for x in range(bx)], xr[0, i], xr[1, i],
            [yr[0, i, x:x + 1] for x in range(bx)], [yr[1, i, x:x + 1] for x in range(bx)],
            [zr[0, x, :, i:i + 1] for x in range(bx)], [zr[1, x, :, i:i + 1] for x in range(bx)])
        for x in range(bx):
            ubuf[i, x] = found[x]
        if (i + 1) % CHUNK == 0:
            face_start(*applied_faces, (0,), (i + 1 - CHUNK, i + 1))
    pack_faces(ubuf, (yhpack, zhpack))
    face_start(*applied_faces, (1, 2), (0, KEEP))
    ufields = [of(ubuf, i) for i in range(KEEP)]
    shares = [jnp.zeros((ROWS, LANES), jnp.float32) for _ in range(2)]
    for j in range(KEEP):
        v = [ubuf[j, x] for x in range(bx)]
        cols = (dots(v, basis_fields[:KEEP] + [of(w_ref), of(image, 0)]),
                dots(v, [None] * (j // 8 * 8) + ufields[j // 8 * 8:]))
        shares = [jnp.where(lane == j, col, part) for col, part in zip(cols, shares)]
    mixed = jnp.zeros((8, LANES), jnp.float32)
    for k in range(6):
        part = shares[k // 3][k % 3 * 8:k % 3 * 8 + 8]
        mixed = mixed + (part if k == 0 else pltpu.roll(part, KEEP * k, 1))
    mix_arrival = total_start(1, mixed)
    halo_wait(1, field_targets(1))
    second = stencil(
        applied, xs[1, 0], xs[1, 1],
        [ys[1, 0, x, by - 1:by, :] for x in range(bx)],
        [ys[1, 1, x, 0:1, :] for x in range(bx)],
        [zs[1, 0, x, :, bz - 1:bz] for x in range(bx)],
        [zs[1, 1, x, :, 0:1] for x in range(bx)],
    )
    for x in range(bx):
        image[1, x] = second[x]
    field_start(2, image.at[1])

    packed = total_end(0, packed, first_arrival)
    packed = jnp.concatenate([packed, pltpu.roll(packed, LANES - 3 * cut, 1)], axis=0)
    gram = jnp.concatenate(
        [packed, pltpu.roll(packed, LANES - cut, 1), pltpu.roll(packed, LANES - 2 * cut, 1)],
        axis=0)
    own = jnp.sum(jnp.where(lane == KEEP, gram, 0.0), axis=1, keepdims=True)
    norm_sq = own[KEEP + 1:KEEP + 2]
    image_sq = own[ROWS - 1:ROWS]
    gram = jnp.where((lane < KEEP) & (row <= KEEP), gram, 0.0)
    next_row = gram[KEEP:KEEP + 1]
    gram = jnp.where(lane == KEEP, as_col(next_row) + jnp.where(row1 == KEEP, norm_sq, 0.0), gram)
    scale = 1.0 / jnp.maximum(jnp.sqrt(norm_sq), 0.5)
    gram = gram * jnp.where(row == KEEP, scale, 1.0) * jnp.where(lane == KEEP, scale, 1.0)
    for x in range(bx):
        out[KEEP, x] = w_ref[x] * scale
    applied = [tile * scale for tile in applied]
    image_sq = image_sq * scale * scale
    own = jnp.where(row1 <= KEEP, own * scale * jnp.where(row1 == KEEP, scale, 1.0), 0.0)

    for x in range(bx):
        abuf[x] = applied[x]
    hcols = []

    def step(count, c_row, c_col, image_sq, gram):
        twice = jnp.where(row == lane, 2.0, 0.0) - gram
        if c_col is None:
            t_col = jnp.sum(twice * c_row, axis=1, keepdims=True)
            t_row = as_row(t_col)
        else:
            t_row = jnp.sum(twice * c_col, axis=0, keepdims=True)
            t_col = as_col(t_row)
        weights = jnp.broadcast_to(t_col, (ROWS, LANES))
        gt_row = jnp.sum(gram * weights, axis=0, keepdims=True)
        length_sq = image_sq + jnp.sum(t_row * (gt_row - 2.0 * c_row), axis=1, keepdims=True)
        length_sq = jnp.maximum(length_sq, 0.0)
        length = jnp.sqrt(length_sq)
        inverse = 1.0 / jnp.maximum(length, 0.5)
        hcols.append(jnp.where(lane1 == count, length, t_row))
        return t_row, t_col, weights, length_sq, inverse

    def less(start, weights, fields):
        for i, field in enumerate(fields):
            weight = jnp.broadcast_to(weights[i:i + 1, :], (by, bz))
            start = [start[x] - weight * field(x) for x in range(bx)]
        return start

    def widen(gram, count, t_row, c_row, length_sq, inverse):
        e_row = t_row - c_row
        e_col = as_col(e_row)
        cross_col = (e_col - jnp.sum(gram * e_row, axis=1, keepdims=True)) * inverse
        cross_row = (e_row - jnp.sum(gram * e_col, axis=0, keepdims=True)) * inverse
        corner = length_sq * inverse * inverse
        gram = jnp.where(row == count, cross_row, jnp.where(lane == count, cross_col, gram))
        return jnp.where((row == count) & (lane == count), corner, gram)

    def pick(values, at):
        return jnp.sum(jnp.where(lane1 == at, values, 0.0), axis=1, keepdims=True)

    count = KEEP + 1
    first_row = as_row(own)
    t_row, t_col, weights, length_sq, inverse = step(count, first_row, own, image_sq, gram)
    newest = [tile * inverse for tile in less(applied, weights, basis_fields[:count])]
    for x in range(bx):
        out[count, x] = newest[x]
    second = [tile * inverse for tile in less(
        [image[1, x] * scale for x in range(bx)], weights, ufields + [of(abuf)])]
    for x in range(bx):
        pbuf[x] = second[x]
    halo_wait(4, (xh, yh, zh))
    halo_wait(2, field_targets(2))
    sides = []
    for side in (0, 1):
        near_row, near_lane = (by - 1, bz - 1) if side == 0 else (0, 0)

        def edge(kind):
            return jnp.concatenate(
                [ys[kind, side, x, near_row:near_row + 1, :] for x in range(bx)], axis=0)

        weight = weights[KEEP:KEEP + 1, :]
        x_part = (xs[2, side] - weight * xs[1, side]) * scale
        y_part = (edge(2) - weight * edge(1)) * scale
        for i in range(KEEP):
            weight = weights[i:i + 1, :]
            x_part = x_part - weight * xh[side, i]
            y_part = y_part - weight * yh[side, i]
        x_part = x_part * inverse
        y_part = y_part * inverse
        z_part = []
        for x in range(bx):
            image_edge, own_edge = (
                zs[kind, side, x, :, near_lane:near_lane + 1] * scale for kind in (2, 1))
            mine = jnp.where(lane3 == KEEP, own_edge, zh[side, x])
            z_part.append(
                (image_edge - jnp.sum(mine * t_row, axis=1, keepdims=True)) * inverse)
        sides.append((x_part, [y_part[x:x + 1] for x in range(bx)], z_part))
    gram = widen(gram, count, t_row, first_row, length_sq, inverse)

    count = KEEP + 2
    grown = ufields + [of(abuf), of(pbuf)]
    p_row = (as_row(dots(second, basis_fields[:count]))
             + as_row(dots(second, grown), 32))
    q_row = as_row(dots(newest, grown[:KEEP + 1]), 32)
    third = stencil(second, sides[0][0], sides[1][0], sides[0][1], sides[1][1],
                    sides[0][2], sides[1][2])
    r_row = (as_row(dots(third, basis_fields[:count]))
             + as_row(dots(third, grown + [lambda x: third[x]]), 32))
    last = jnp.concatenate([p_row, r_row, q_row], axis=0)
    earlier = pending[:]
    pending.clear()
    last_arrival = total_start(2, last)
    for copy in earlier:
        copy.wait()
    halo_finish()
    mixed = total_end(1, mixed, mix_arrival)
    parts = [jnp.where(lane8 < KEEP,
                       mixed if k == 0 else pltpu.roll(mixed, LANES - KEEP * k, 1), 0.0)
             for k in range(6)]
    across = jnp.concatenate(parts[0:3], axis=0)
    inside = jnp.concatenate(parts[3:6], axis=0)
    image_row = across[KEEP + 1:KEEP + 2] * scale
    across = jnp.where(row < KEEP, across, jnp.where(row == KEEP, across * scale, 0.0))
    across = jnp.where((lane == KEEP) & (row <= KEEP), own, across)
    inside = inside * jnp.where(row // 8 > lane // 8, 2.0, 1.0)
    inside = jnp.where(row == KEEP, jnp.where(lane == KEEP, image_sq, 2.0 * image_row), inside)

    last = total_end(2, last, last_arrival)
    shifted_last = pltpu.roll(last, LANES - 32, 1)
    c_row = jnp.where(lane1 < count, last[0:1], 0.0)
    pz_row = jnp.where(lane1 < count, shifted_last[0:1], 0.0)
    rq_row = jnp.where(lane1 < count, last[1:2], 0.0)
    rz_row = jnp.where(lane1 <= count, shifted_last[1:2], 0.0)
    qz_row = jnp.where(lane1 < KEEP + 1, shifted_last[2:3], 0.0)
    across = jnp.where(row == KEEP + 1, qz_row, across)
    across = jnp.where((lane == KEEP + 1) & (row < count), as_col(c_row), across)
    inside = jnp.where(row == KEEP + 1,
                       jnp.where(lane == KEEP + 1, pz_row, 2.0 * pz_row), inside)
    t_row, t_col, weights, length_sq, inverse = step(
        count, c_row, None, pick(pz_row, KEEP + 1), gram)
    gram = widen(gram, count, t_row, c_row, length_sq, inverse)
    h_col = jnp.sum(jnp.where(row == lane, rq_row, 0.0) - across * t_row, axis=1, keepdims=True)
    th = jnp.sum(t_col * h_col, axis=0, keepdims=True)
    corner = jnp.sum(jnp.where(lane1 == KEEP + 1, rz_row, 0.0) - pz_row * t_row,
                     axis=1, keepdims=True)
    corner = (corner - th) * inverse * inverse
    wt_row = jnp.sum(inside * t_col, axis=0, keepdims=True)
    image_sq = jnp.sum(
        jnp.where(lane1 == count, rz_row, (wt_row - 2.0 * rz_row) * t_row),
        axis=1, keepdims=True) * inverse * inverse
    c_col = jnp.where(row1 < count, h_col * inverse, jnp.where(row1 == count, corner, 0.0))
    newest = [tile * inverse for tile in less(second, weights, basis_fields[:count])]
    for x in range(bx):
        out[count, x] = newest[x]
    applied = [tile * inverse for tile in less(third, weights, grown)]
    count = KEEP + 3
    t_row, t_col, weights, length_sq, inverse = step(count, as_row(c_col), c_col, image_sq, gram)
    newest = [tile * inverse for tile in less(applied, weights, basis_fields[:count])]
    for x in range(bx):
        out[count, x] = newest[x]

    for k in range(EXPAND):
        hess[k:k + 1] = hcols[k]
    finish_sends()


def per_device(krylov_basis, schur_vectors, next_vector, diag_shift, velocity):
    sizes = tuple(lax.axis_size(a) for a in AXES)
    block = next_vector.shape
    bx, by, bz = block
    cells = float(bx * by * bz * sizes[0] * sizes[1] * sizes[2])
    n0, n1 = sizes[1] * sizes[2], sizes[0]
    nrow = n0 * n1 if n0 * n1 <= DIRECT else n0
    f32 = jnp.float32
    vmem = pl.BlockSpec(memory_space=pltpu.VMEM)
    dma = pltpu.SemaphoreType.DMA
    vectors, columns = pl.pallas_call(
        functools.partial(body, sizes, cells),
        out_shape=(
            pltpu.VMEM((ROWS,) + block, f32),
            pltpu.VMEM((8, LANES), f32),
        ),
        in_specs=[
            pl.BlockSpec(memory_space=pl.ANY) for _ in range(5)
        ],
        out_specs=(vmem, vmem),
        scratch_shapes=[
            pltpu.VMEM(schur_vectors.shape[::-1], f32),
            pltpu.VMEM(block, f32),
            pltpu.VMEM(block, f32),
            pltpu.VMEM((3,) + block, f32),
            pltpu.VMEM(((krylov_basis.shape[0] + 15) // 16 * 16,) + block, f32),
            pltpu.VMEM((2,) + block, f32),
            pltpu.VMEM((2, KEEP, by, bz), f32),
            pltpu.VMEM((2, KEEP, bx, bz), f32),
            pltpu.VMEM((2,) + block, f32),
            pltpu.VMEM((2, KEEP, bx, bz), f32),
            pltpu.VMEM((2,) + block, f32),
            pltpu.VMEM((2, KEEP, by, bz), f32),
            pltpu.VMEM((2, KEEP, bx, bz), f32),
            pltpu.VMEM((2,) + block, f32),
            pltpu.VMEM((2, KEEP, bx, bz), f32),
            pltpu.VMEM((2,) + block, f32),
            pltpu.VMEM((EXPAND, 2, by, bz), f32),
            pltpu.VMEM((EXPAND, 2) + block, f32),
            pltpu.VMEM((EXPAND, 2) + block, f32),
            *[pltpu.VMEM(shape, f32) for k, rows in enumerate((4, 8, 3)) for shape in (
                (rows, LANES), ((n0 if k == MIX else nrow) - 1, rows, LANES), (rows, LANES),
                (n1 - 1, rows, LANES))],
            pltpu.VMEM((KEEP,) + block, f32),
            pltpu.VMEM(block, f32),
            pltpu.VMEM(block, f32),
            dma((5,)), dma((3,)), dma((5, 3)),
            dma((6,)), dma((2 if nrow > n0 else 6,)),
            pltpu.SemaphoreType.REGULAR((max(turns_of(sizes[0]), 1), 2 * NEAR)),
        ],
        compiler_params=pltpu.CompilerParams(collective_id=0, has_side_effects=True),
    )(krylov_basis, schur_vectors.T, next_vector, diag_shift, velocity)
    return vectors, columns[0:EXPAND, 0:ROWS].T


def solution(mesh):
    in_specs = (
        P(None, "gx", "gy", "gz"),
        P(),
        P("gx", "gy", "gz"),
        P("gx", "gy", "gz"),
        P(None, "gx", "gy", "gz"),
    )
    out_specs = (P(None, "gx", "gy", "gz"), P())
    return jax.shard_map(
        per_device, mesh=mesh, in_specs=in_specs, out_specs=out_specs, check_vma=False
    )
```

```python
import functools
import math

import jax
import jax.numpy as jnp
from jax import lax
from jax.experimental import pallas as pl
from jax.experimental.pallas import tpu as pltpu
from jax.sharding import PartitionSpec as P

KEEP = 20
EXPAND = 3
ROWS = 24
LANES = 128
DIRECT = 64
CHUNK = 5
MIX = 1
NEAR = 2
AXES = ("gx", "gy", "gz")


def turns_of(line):
    return -(-max(line - 2, 0) // NEAR) + 1 if line > 1 else 0


def partner_steps(phase, sizes):
    xs = range(1, sizes[0]) if phase else ()
    steps = [(dx, 0, 0) for dx in xs] if phase == 1 else [
        (dx, dy, dz) for dx in tuple(reversed(xs)) + (0,)
        for dy in range(sizes[1]) for dz in range(sizes[2])]
    return [step for step in steps if step != (0, 0, 0)]


def body(
    sizes, cells,
    kry_hbm, schur_hbm, w_hbm, diag_hbm, vel_hbm,
    out, hess,
    schur, w_ref, diag, vel, kry, image, xr, yr, zr, ypack, zpack, xh, yh, zh, yhpack, zhpack, xs, ys, zs,
    rsend, rrecv0, rmid, rrecv1, msend, mrecv0, mmid, mrecv1, lsend, lrecv0, lmid, lrecv1,
    ubuf, abuf, pbuf,
    load_sem, halo_send, halo_recv, sums_sem, line_sem, ready,
):
    place = tuple(lax.axis_index(a) for a in AXES)
    basis = kry_hbm.shape[0]
    bx, by, bz = w_ref.shape
    loads = [
        pltpu.make_async_copy(source, target, load_sem.at[k])
        for k, (source, target) in enumerate((
            (w_hbm, w_ref), (schur_hbm, schur), (kry_hbm, kry.at[0:basis]), (diag_hbm, diag),
            (vel_hbm, vel)))
    ]
    for copy in loads:
        copy.start()
    direct = sizes[0] * sizes[1] * sizes[2] <= DIRECT
    shifted = [[lax.rem(place[d] + k, sizes[d]) for k in range(sizes[d])] for d in range(3)]

    def partners(phase):
        return [tuple(shifted[d][step[d]] for d in range(3))
                for step in partner_steps(phase, sizes)]


    for ref in (xr, yr, zr, xh, yh, zh, xs, ys, zs):
        ref[...] = jnp.zeros_like(ref)

    barrier = pltpu.get_barrier_semaphore()
    line = [
        ((place[0] + step,) + place[1:],
         place[0] < sizes[0] - step if step > 0 else place[0] >= -step)
        for far in range(1, min(NEAR, sizes[0] - 1) + 1) for step in (far, -far)]

    def tell(semaphore, to):
        pl.semaphore_signal(
            semaphore, inc=1, device_id=to, device_id_type=pl.DeviceIdType.MESH)

    for to in partners(0) + ([] if direct else partners(1)):
        tell(barrier, to)
    if direct:
        for to, near in line:
            pl.when(near)(functools.partial(tell, barrier, to))
    turns_needed = turns_of(sizes[0]) if direct else 0

    def pass_on(turn):
        if 0 < turn <= turns_needed:
            for side, (to, near) in enumerate(line if turn < turns_needed else line[:2]):
                pl.when(near)(functools.partial(pl.semaphore_wait, ready.at[turn - 1, side], 1))
        if turn < turns_needed:
            for side, (to, near) in enumerate(line if turn + 1 < turns_needed else line[:2]):
                pl.when(near)(functools.partial(tell, ready.at[turn, side ^ 1], to))


    sent = [[] for _ in range(3)]

    def halo_start(kind, dims, sources, targets):
        for d in dims:
            for side in (0, 1):
                to = list(place)
                to[d] = place[d] + (1 if side == 0 else -1)
                can_send = place[d] < sizes[d] - 1 if side == 0 else place[d] > 0
                source = sources[d][side]
                sent[d].append(math.prod(source.shape))
                pl.when(can_send)(pltpu.make_async_remote_copy(
                    src_ref=source, dst_ref=targets[d][side],
                    send_sem=halo_send.at[d], recv_sem=halo_recv.at[kind, d],
                    device_id=tuple(to), device_id_type=pl.DeviceIdType.MESH).start)

    def landed(ref, semaphore):
        pltpu.make_async_copy(ref, ref, semaphore).wait()

    def halo_wait(kind, targets):
        for d in range(3):
            before, after = place[d] > 0, place[d] < sizes[d] - 1
            semaphore = halo_recv.at[kind, d]
            if sizes[d] > 2:
                pl.when(before & after)(functools.partial(landed, targets[d], semaphore))
                pl.when(before != after)(functools.partial(landed, targets[d].at[0], semaphore))
            elif sizes[d] == 2:
                landed(targets[d].at[0], semaphore)

    def halo_finish():
        for d in range(3):
            before, after = place[d] > 0, place[d] < sizes[d] - 1
            tiles = sum(sent[d]) // 2 // (by * bz)
            if sizes[d] > 2:
                pl.when(before & after)(functools.partial(
                    landed, kry.at[0:tiles, 0:2], halo_send.at[d]))
                pl.when(before != after)(functools.partial(
                    landed, kry.at[0:tiles, 0], halo_send.at[d]))
            elif sizes[d] == 2:
                landed(kry.at[0:tiles, 0], halo_send.at[d])

    def field_targets(kind):
        return tuple(r.at[kind] for r in (xs, ys, zs))

    def field_start(kind, ref):
        halo_start(kind, range(3), ((ref.at[bx - 1], ref.at[0]), (ref, ref), (ref, ref)),
                   tuple((r.at[0], r.at[1]) for r in field_targets(kind)))

    def exchange(send, slots, sem_s, sem_r, phase):
        for at, to in enumerate(partners(phase)):
            pltpu.make_async_remote_copy(
                src_ref=send, dst_ref=slots.at[at], send_sem=sem_s, recv_sem=sem_r,
                device_id=to, device_id_type=pl.DeviceIdType.MESH,
            ).start()
        pending.append(pltpu.make_async_copy(slots, slots, sem_s))
        return pltpu.make_async_copy(slots, slots, sem_r)

    def gather_sum(arrival, own, slots):
        arrival.wait()
        terms = [own] + [slots[k] for k in range(slots.shape[0])]
        while len(terms) > 1:
            terms = [sum(terms[k + 1:k + 2], terms[k]) for k in range(0, len(terms), 2)]
        return terms[0]

    pending = []

    def finish_sends():
        while pending:
            pending.pop().wait()

    groups = (
        (rsend, rrecv0, rmid, rrecv1), (msend, mrecv0, mmid, mrecv1), (lsend, lrecv0, lmid, lrecv1))

    def total_start(k, value):
        send, first = groups[k][:2]
        send[...] = value
        return exchange(send, first, sums_sem.at[2 * k], sums_sem.at[2 * k + 1],
                        2 if direct and k != MIX else 0)

    def total_end(k, value, arrival):
        first, between, second = groups[k][1:]
        value = gather_sum(arrival, value, first)
        if not direct or k == MIX:
            at = 0 if direct else k
            between[...] = value
            arrival = exchange(between, second, line_sem.at[2 * at], line_sem.at[2 * at + 1], 1)
            value = gather_sum(arrival, value, second)
        return value * (1.0 / cells)

    lane3 = lax.broadcasted_iota(jnp.int32, (by, bz), 1)
    row3 = lax.broadcasted_iota(jnp.int32, (by, bz), 0)

    def stencil(v, x_before, x_after, y_before, y_after, z_before, z_after):
        res = []
        for x in range(bx):
            here = v[x]
            xb = v[x - 1] if x > 0 else x_before
            xa = v[x + 1] if x < bx - 1 else x_after
            yb = jnp.where(row3 == 0, y_before[x], pltpu.roll(here, 1, 0))
            ya = jnp.where(row3 == by - 1, y_after[x], pltpu.roll(here, by - 1, 0))
            zb = jnp.where(lane3 == 0, z_before[x], pltpu.roll(here, 1, 1))
            za = jnp.where(lane3 == bz - 1, z_after[x], pltpu.roll(here, bz - 1, 1))
            neighbours = xa + xb + ya + yb + za + zb
            flow = (vel[0, x] * (xa - xb) + vel[1, x] * (ya - yb) + vel[2, x] * (za - zb))
            res.append((6.0 + diag[x]) * here - neighbours + 0.5 * flow)
        return res

    row8 = lax.broadcasted_iota(jnp.int32, (8, LANES), 0)

    def fold(tiles):
        for half in (4, 2, 1):
            low = (row8 & half) == 0
            tiles = [
                jnp.where(low, tiles[k] + pltpu.roll(tiles[k], 8 - half, 0),
                          tiles[k + half] + pltpu.roll(tiles[k + half], half, 0))
                for k in range(half)]
        return tiles[0]

    def dots(v, fields):
        groups = []
        for first in range(0, ROWS, 8):
            tiles = []
            for k in range(first, first + 8):
                field = fields[k] if k < len(fields) else None
                if field is None:
                    tiles.append(None)
                    continue
                total = field(0) * v[0]
                for x in range(1, bx):
                    total = total + field(x) * v[x]
                if by > 8:
                    total = sum(total[8 * t:8 * t + 8] for t in range(1, by // 8)) + total[0:8]
                tiles.append(total)
            if all(tile is None for tile in tiles):
                groups.append(jnp.zeros((8, bz), jnp.float32))
            else:
                groups.append(fold([
                    jnp.zeros((8, bz), jnp.float32) if t is None else t for t in tiles]))
        return jnp.sum(jnp.concatenate(groups, axis=0), axis=1, keepdims=True)

    def of(ref, *at):
        return lambda x: ref[at + (x,)]

    basis_fields = [of(out, i) for i in range(ROWS)]

    loads[0].wait()

    out[KEEP + 1:ROWS] = jnp.zeros((ROWS - KEEP - 1, bx, by, bz), jnp.float32)
    out[KEEP] = w_ref[...]
    deep = kry.shape[0]
    for i in range(basis, deep):
        kry[i] = jnp.zeros((bx, by, bz), jnp.float32)
    loads[1].wait()

    def halves(value):
        high = value.astype(jnp.bfloat16).astype(jnp.float32)
        return high, value - high

    def times(a, b):
        return lax.dot_general(a, b, (((1,), (0,)), ((), ())),
                               precision=lax.Precision.DEFAULT,
                               preferred_element_type=jnp.float32)

    spread = (lax.broadcasted_iota(jnp.int32, (basis, deep * by), 1) // by
              == lax.broadcasted_iota(jnp.int32, (basis, deep * by), 0)).astype(jnp.float32)
    same = (lax.broadcasted_iota(jnp.int32, (by, deep * by), 1) % by
            == lax.broadcasted_iota(jnp.int32, (by, deep * by), 0))
    turns = []
    for part in halves(schur[...]):
        wide = times(part, spread)
        turns.append(jnp.concatenate(
            [jnp.where(same, jnp.broadcast_to(wide[j:j + 1], same.shape), 0.0)
             for j in range(KEEP)], axis=0))
    both = jnp.concatenate(turns, axis=0)
    loads[2].wait()
    for x in range(0, bx, 2):
        pair = range(x, min(x + 2, bx))
        tiles = jnp.concatenate([kry[:, k].reshape(deep * by, bz) for k in pair], axis=1)
        high, low = halves(tiles)
        first = times(both, high)
        found = first[:KEEP * by] + (first[KEEP * by:] + times(turns[0], low))
        for j in range(KEEP):
            for k in pair:
                out[j, k] = found[j * by:(j + 1) * by, (k - x) * bz:(k - x + 1) * bz]

    pl.semaphore_wait(barrier, len(partners(0)) + (
        sum(near.astype(jnp.int32) for _, near in line) if direct else len(partners(1))))
    field_start(0, w_ref)
    pass_on(0)

    def face_start(kind, ref, packs, targets, dims, span):
        (ys_, zs_), (first, last) = packs, span
        halo_start(
            kind, dims,
            ((ref.at[first:last, bx - 1], ref.at[first:last, 0]), (ys_.at[0], ys_.at[1]),
             (zs_.at[0], zs_.at[1])),
            tuple((r.at[0, first:last], r.at[1, first:last]) if d == 0 else (r.at[0], r.at[1])
                  for d, r in enumerate(targets)))

    def pack_faces(ref, packs):
        ys_, zs_ = packs
        for side, (near, edge) in enumerate(((by - 1, bz - 1), (0, 0))):
            for i in range(KEEP):
                ys_[side, i] = ref[i, :, near, :]
            for x in range(bx):
                face = jnp.zeros((by, bz), jnp.float32)
                for i in range(KEEP):
                    face = jnp.where(
                        lane3 == i, pltpu.roll(ref[i, x], (i - edge) % bz, 1), face)
                zs_[side, x] = face

    turned = (3, out, (ypack, zpack), (xr, yr, zr))
    face_start(*turned, (0,), (0, KEEP))
    pack_faces(out, (ypack, zpack))
    face_start(*turned, (1, 2), (0, KEEP))
    pass_on(1)

    row = lax.broadcasted_iota(jnp.int32, (ROWS, LANES), 0)
    lane = lax.broadcasted_iota(jnp.int32, (ROWS, LANES), 1)
    lane1 = lax.broadcasted_iota(jnp.int32, (1, LANES), 1)
    row1 = lax.broadcasted_iota(jnp.int32, (ROWS, 1), 0)

    def as_row(col, shift=0):
        return jnp.sum(jnp.where(row + shift == lane, col, 0.0), axis=0, keepdims=True)

    def as_col(values):
        return jnp.sum(jnp.where(row == lane, values, 0.0), axis=1, keepdims=True)

    gram = jnp.zeros((ROWS, LANES), jnp.float32)
    for j in range(KEEP + 1):
        col = dots([out[j, x] for x in range(bx)],
                   [None] * (j // 8 * 8) + basis_fields[j // 8 * 8:KEEP + 1])
        gram = jnp.where((lane == j) & (row < KEEP + 1), col, gram)
    lane8 = lax.broadcasted_iota(jnp.int32, (8, LANES), 1)
    below = jnp.where(row // 8 > lane // 8, gram, 0.0)
    gram = gram + jnp.concatenate(
        [below, jnp.zeros((LANES - ROWS, LANES), jnp.float32)], axis=0).T[0:ROWS]

    loads[3].wait()
    loads[4].wait()
    halo_wait(0, field_targets(0))
    applied = stencil(
        [w_ref[x] for x in range(bx)], xs[0, 0], xs[0, 1],
        [ys[0, 0, x, by - 1:by, :] for x in range(bx)],
        [ys[0, 1, x, 0:1, :] for x in range(bx)],
        [zs[0, 0, x, :, bz - 1:bz] for x in range(bx)],
        [zs[0, 1, x, :, 0:1] for x in range(bx)],
    )
    for x in range(bx):
        image[0, x] = applied[x]
    field_start(1, image.at[0])
    own_sq = jnp.sum(jnp.where((row == KEEP) & (lane == KEEP), gram, 0.0),
                     axis=0, keepdims=True)
    own_sq = jnp.sum(own_sq, axis=1, keepdims=True)
    own = dots(applied, basis_fields[:KEEP + 1] + [None, None, of(image, 0)])
    own = jnp.where(row1 == KEEP + 1, own_sq, own)
    gram = jnp.where(lane < KEEP, gram, jnp.where(lane == KEEP, own, 0.0))
    cut = KEEP + 1
    packed = gram[0:8] + pltpu.roll(gram[8:16], cut, 1) + pltpu.roll(gram[16:24], 2 * cut, 1)
    packed = packed[0:4] + pltpu.roll(packed[4:8], 3 * cut, 1)
    for turn in range(2, turns_needed + 1):
        pass_on(turn)
    first_arrival = total_start(0, packed)

    halo_wait(3, (xr, yr, zr))
    applied_faces = (4, ubuf, (yhpack, zhpack), (xh, yh, zh))
    for i in range(KEEP):
        found = stencil(
            [out[i, x] for x in range(bx)], xr[0, i], xr[1, i],
            [yr[0, i, x:x + 1] for x in range(bx)], [yr[1, i, x:x + 1] for x in range(bx)],
            [zr[0, x, :, i:i + 1] for x in range(bx)], [zr[1, x, :, i:i + 1] for x in range(bx)])
        for x in range(bx):
            ubuf[i, x] = found[x]
        if (i + 1) % CHUNK == 0:
            face_start(*applied_faces, (0,), (i + 1 - CHUNK, i + 1))
    pack_faces(ubuf, (yhpack, zhpack))
    face_start(*applied_faces, (1, 2), (0, KEEP))
    ufields = [of(ubuf, i) for i in range(KEEP)]
    def table(fields):
        part = jnp.zeros((ROWS, LANES), jnp.float32)
        for j in range(KEEP):
            part = jnp.where(
                lane == j, dots([ubuf[j, x] for x in range(bx)], fields(j)), part)
        return part

    shares = [table(lambda j: basis_fields[:KEEP] + [of(w_ref), of(image, 0)])]
    halo_wait(1, field_targets(1))
    second = stencil(
        applied, xs[1, 0], xs[1, 1],
        [ys[1, 0, x, by - 1:by, :] for x in range(bx)],
        [ys[1, 1, x, 0:1, :] for x in range(bx)],
        [zs[1, 0, x, :, bz - 1:bz] for x in range(bx)],
        [zs[1, 1, x, :, 0:1] for x in range(bx)],
    )
    for x in range(bx):
        image[1, x] = second[x]
    field_start(2, image.at[1])

    shares.append(table(lambda j: [None] * (j // 8 * 8) + ufields[j // 8 * 8:]))
    mixed = jnp.zeros((8, LANES), jnp.float32)
    for k in range(6):
        part = shares[k // 3][k % 3 * 8:k % 3 * 8 + 8]
        mixed = mixed + (part if k == 0 else pltpu.roll(part, KEEP * k, 1))
    mix_arrival = total_start(1, mixed)
    packed = total_end(0, packed, first_arrival)
    packed = jnp.concatenate([packed, pltpu.roll(packed, LANES - 3 * cut, 1)], axis=0)
    gram = jnp.concatenate(
        [packed, pltpu.roll(packed, LANES - cut, 1), pltpu.roll(packed, LANES - 2 * cut, 1)],
        axis=0)
    own = jnp.sum(jnp.where(lane == KEEP, gram, 0.0), axis=1, keepdims=True)
    norm_sq = own[KEEP + 1:KEEP + 2]
    image_sq = own[ROWS - 1:ROWS]
    gram = jnp.where((lane < KEEP) & (row <= KEEP), gram, 0.0)
    next_row = gram[KEEP:KEEP + 1]
    gram = jnp.where(lane == KEEP, as_col(next_row) + jnp.where(row1 == KEEP, norm_sq, 0.0), gram)
    scale = 1.0 / jnp.maximum(jnp.sqrt(norm_sq), 0.5)
    gram = gram * jnp.where(row == KEEP, scale, 1.0) * jnp.where(lane == KEEP, scale, 1.0)
    for x in range(bx):
        out[KEEP, x] = w_ref[x] * scale
    applied = [tile * scale for tile in applied]
    image_sq = image_sq * scale * scale
    own = jnp.where(row1 <= KEEP, own * scale * jnp.where(row1 == KEEP, scale, 1.0), 0.0)

    for x in range(bx):
        abuf[x] = applied[x]
    hcols = []

    def step(count, c_row, c_col, image_sq, gram):
        twice = jnp.where(row == lane, 2.0, 0.0) - gram
        if c_col is None:
            t_col = jnp.sum(twice * c_row, axis=1, keepdims=True)
            t_row = as_row(t_col)
        else:
            t_row = jnp.sum(twice * c_col, axis=0, keepdims=True)
            t_col = as_col(t_row)
        weights = jnp.broadcast_to(t_col, (ROWS, LANES))
        gt_row = jnp.sum(gram * weights, axis=0, keepdims=True)
        length_sq = image_sq + jnp.sum(t_row * (gt_row - 2.0 * c_row), axis=1, keepdims=True)
        length_sq = jnp.maximum(length_sq, 0.0)
        length = jnp.sqrt(length_sq)
        inverse = 1.0 / jnp.maximum(length, 0.5)
        hcols.append(jnp.where(lane1 == count, length, t_row))
        return t_row, t_col, weights, length_sq, inverse

    def less(start, weights, fields):
        for i, field in enumerate(fields):
            weight = jnp.broadcast_to(weights[i:i + 1, :], (by, bz))
            start = [start[x] - weight * field(x) for x in range(bx)]
        return start

    def widen(gram, count, t_row, c_row, length_sq, inverse):
        e_row = t_row - c_row
        e_col = as_col(e_row)
        cross_col = (e_col - jnp.sum(gram * e_row, axis=1, keepdims=True)) * inverse
        cross_row = (e_row - jnp.sum(gram * e_col, axis=0, keepdims=True)) * inverse
        corner = length_sq * inverse * inverse
        gram = jnp.where(row == count, cross_row, jnp.where(lane == count, cross_col, gram))
        return jnp.where((row == count) & (lane == count), corner, gram)

    def pick(values, at):
        return jnp.sum(jnp.where(lane1 == at, values, 0.0), axis=1, keepdims=True)

    count = KEEP + 1
    first_row = as_row(own)
    t_row, t_col, weights, length_sq, inverse = step(count, first_row, own, image_sq, gram)
    newest = [tile * inverse for tile in less(applied, weights, basis_fields[:count])]
    for x in range(bx):
        out[count, x] = newest[x]
    second = [tile * inverse for tile in less(
        [image[1, x] * scale for x in range(bx)], weights, ufields + [of(abuf)])]
    for x in range(bx):
        pbuf[x] = second[x]
    halo_wait(4, (xh, yh, zh))
    halo_wait(2, field_targets(2))
    sides = []
    for side in (0, 1):
        near_row, near_lane = (by - 1, bz - 1) if side == 0 else (0, 0)

        def edge(kind):
            return jnp.concatenate(
                [ys[kind, side, x, near_row:near_row + 1, :] for x in range(bx)], axis=0)

        weight = weights[KEEP:KEEP + 1, :]
        x_part = (xs[2, side] - weight * xs[1, side]) * scale
        y_part = (edge(2) - weight * edge(1)) * scale
        for i in range(KEEP):
            weight = weights[i:i + 1, :]
            x_part = x_part - weight * xh[side, i]
            y_part = y_part - weight * yh[side, i]
        x_part = x_part * inverse
        y_part = y_part * inverse
        z_part = []
        for x in range(bx):
            image_edge, own_edge = (
                zs[kind, side, x, :, near_lane:near_lane + 1] * scale for kind in (2, 1))
            mine = jnp.where(lane3 == KEEP, own_edge, zh[side, x])
            z_part.append(
                (image_edge - jnp.sum(mine * t_row, axis=1, keepdims=True)) * inverse)
        sides.append((x_part, [y_part[x:x + 1] for x in range(bx)], z_part))
    gram = widen(gram, count, t_row, first_row, length_sq, inverse)

    count = KEEP + 2
    grown = ufields + [of(abuf), of(pbuf)]
    p_row = (as_row(dots(second, basis_fields[:count]))
             + as_row(dots(second, grown), 32))
    q_row = as_row(dots(newest, grown[:KEEP + 1]), 32)
    third = stencil(second, sides[0][0], sides[1][0], sides[0][1], sides[1][1],
                    sides[0][2], sides[1][2])
    r_row = (as_row(dots(third, basis_fields[:count]))
             + as_row(dots(third, grown + [lambda x: third[x]]), 32))
    last = jnp.concatenate([p_row, r_row, q_row], axis=0)
    earlier = pending[:]
    pending.clear()
    last_arrival = total_start(2, last)
    for copy in earlier:
        copy.wait()
    halo_finish()
    mixed = total_end(1, mixed, mix_arrival)
    parts = [jnp.where(lane8 < KEEP,
                       mixed if k == 0 else pltpu.roll(mixed, LANES - KEEP * k, 1), 0.0)
             for k in range(6)]
    across = jnp.concatenate(parts[0:3], axis=0)
    inside = jnp.concatenate(parts[3:6], axis=0)
    image_row = across[KEEP + 1:KEEP + 2] * scale
    across = jnp.where(row < KEEP, across, jnp.where(row == KEEP, across * scale, 0.0))
    across = jnp.where((lane == KEEP) & (row <= KEEP), own, across)
    inside = inside * jnp.where(row // 8 > lane // 8, 2.0, 1.0)
    inside = jnp.where(row == KEEP, jnp.where(lane == KEEP, image_sq, 2.0 * image_row), inside)

    last = total_end(2, last, last_arrival)
    shifted_last = pltpu.roll(last, LANES - 32, 1)
    c_row = jnp.where(lane1 < count, last[0:1], 0.0)
    pz_row = jnp.where(lane1 < count, shifted_last[0:1], 0.0)
    rq_row = jnp.where(lane1 < count, last[1:2], 0.0)
    rz_row = jnp.where(lane1 <= count, shifted_last[1:2], 0.0)
    qz_row = jnp.where(lane1 < KEEP + 1, shifted_last[2:3], 0.0)
    across = jnp.where(row == KEEP + 1, qz_row, across)
    across = jnp.where((lane == KEEP + 1) & (row < count), as_col(c_row), across)
    inside = jnp.where(row == KEEP + 1,
                       jnp.where(lane == KEEP + 1, pz_row, 2.0 * pz_row), inside)
    t_row, t_col, weights, length_sq, inverse = step(
        count, c_row, None, pick(pz_row, KEEP + 1), gram)
    gram = widen(gram, count, t_row, c_row, length_sq, inverse)
    h_col = jnp.sum(jnp.where(row == lane, rq_row, 0.0) - across * t_row, axis=1, keepdims=True)
    th = jnp.sum(t_col * h_col, axis=0, keepdims=True)
    corner = jnp.sum(jnp.where(lane1 == KEEP + 1, rz_row, 0.0) - pz_row * t_row,
                     axis=1, keepdims=True)
    corner = (corner - th) * inverse * inverse
    wt_row = jnp.sum(inside * t_col, axis=0, keepdims=True)
    image_sq = jnp.sum(
        jnp.where(lane1 == count, rz_row, (wt_row - 2.0 * rz_row) * t_row),
        axis=1, keepdims=True) * inverse * inverse
    c_col = jnp.where(row1 < count, h_col * inverse, jnp.where(row1 == count, corner, 0.0))
    newest = [tile * inverse for tile in less(second, weights, basis_fields[:count])]
    for x in range(bx):
        out[count, x] = newest[x]
    applied = [tile * inverse for tile in less(third, weights, grown)]
    count = KEEP + 3
    t_row, t_col, weights, length_sq, inverse = step(count, as_row(c_col), c_col, image_sq, gram)
    newest = [tile * inverse for tile in less(applied, weights, basis_fields[:count])]
    for x in range(bx):
        out[count, x] = newest[x]

    for k in range(EXPAND):
        hess[k:k + 1] = hcols[k][:, 0:ROWS]
    finish_sends()


def hand_out(vectors, columns, vectors_hbm, columns_hbm, semaphores):
    copies = [
        pltpu.make_async_copy(source, target, semaphores.at[k])
        for k, (source, target) in enumerate(((vectors, vectors_hbm), (columns, columns_hbm)))]
    for copy in copies:
        copy.start()
    for copy in copies:
        copy.wait()


def per_device(krylov_basis, schur_vectors, next_vector, diag_shift, velocity):
    sizes = tuple(lax.axis_size(a) for a in AXES)
    block = next_vector.shape
    bx, by, bz = block
    cells = float(bx * by * bz * sizes[0] * sizes[1] * sizes[2])
    n0, n1 = sizes[1] * sizes[2], sizes[0]
    nrow = n0 * n1 if n0 * n1 <= DIRECT else n0
    f32 = jnp.float32
    vmem = pl.BlockSpec(memory_space=pltpu.VMEM)
    dma = pltpu.SemaphoreType.DMA
    vectors, columns = pl.pallas_call(
        functools.partial(body, sizes, cells),
        out_shape=(
            pltpu.VMEM((ROWS,) + block, f32),
            pltpu.VMEM((EXPAND, ROWS), f32),
        ),
        in_specs=[
            pl.BlockSpec(memory_space=pl.ANY) for _ in range(5)
        ],
        out_specs=(vmem, vmem),
        scratch_shapes=[
            pltpu.VMEM(schur_vectors.shape[::-1], f32),
            pltpu.VMEM(block, f32),
            pltpu.VMEM(block, f32),
            pltpu.VMEM((3,) + block, f32),
            pltpu.VMEM(((krylov_basis.shape[0] + 15) // 16 * 16,) + block, f32),
            pltpu.VMEM((2,) + block, f32),
            pltpu.VMEM((2, KEEP, by, bz), f32),
            pltpu.VMEM((2, KEEP, bx, bz), f32),
            pltpu.VMEM((2,) + block, f32),
            pltpu.VMEM((2, KEEP, bx, bz), f32),
            pltpu.VMEM((2,) + block, f32),
            pltpu.VMEM((2, KEEP, by, bz), f32),
            pltpu.VMEM((2, KEEP, bx, bz), f32),
            pltpu.VMEM((2,) + block, f32),
            pltpu.VMEM((2, KEEP, bx, bz), f32),
            pltpu.VMEM((2,) + block, f32),
            pltpu.VMEM((EXPAND, 2, by, bz), f32),
            pltpu.VMEM((EXPAND, 2) + block, f32),
            pltpu.VMEM((EXPAND, 2) + block, f32),
            *[pltpu.VMEM(shape, f32) for k, rows in enumerate((4, 8, 3)) for shape in (
                (rows, LANES), ((n0 if k == MIX else nrow) - 1, rows, LANES), (rows, LANES),
                (n1 - 1, rows, LANES))],
            pltpu.VMEM((KEEP,) + block, f32),
            pltpu.VMEM(block, f32),
            pltpu.VMEM(block, f32),
            dma((5,)), dma((3,)), dma((5, 3)),
            dma((6,)), dma((2 if nrow > n0 else 6,)),
            pltpu.SemaphoreType.REGULAR((max(turns_of(sizes[0]), 1), 2 * NEAR)),
        ],
        compiler_params=pltpu.CompilerParams(collective_id=0, has_side_effects=True),
    )(krylov_basis, schur_vectors.T, next_vector, diag_shift, velocity)
    results = [pltpu.with_memory_space_constraint(r, pltpu.VMEM) for r in (vectors, columns)]
    vectors, columns = pl.pallas_call(
        hand_out,
        out_shape=[jax.ShapeDtypeStruct(r.shape, f32) for r in results],
        in_specs=[vmem, vmem],
        out_specs=[pl.BlockSpec(memory_space=pl.ANY)] * 2,
        scratch_shapes=[dma((2,))],
    )(*results)
    return vectors, columns.T


def solution(mesh):
    in_specs = (
        P(None, "gx", "gy", "gz"),
        P(),
        P("gx", "gy", "gz"),
        P("gx", "gy", "gz"),
        P(None, "gx", "gy", "gz"),
    )
    out_specs = (P(None, "gx", "gy", "gz"), P())
    return jax.shard_map(
        per_device, mesh=mesh, in_specs=in_specs, out_specs=out_specs, check_vma=False
    )
```

```python
import functools
import math

import jax
import jax.numpy as jnp
from jax import lax
from jax.experimental import pallas as pl
from jax.experimental.pallas import tpu as pltpu
from jax.sharding import PartitionSpec as P

KEEP = 20
EXPAND = 3
ROWS = 24
LANES = 128
DIRECT = 64
CHUNK = 5
MIX = 1
NEAR = 2
AXES = ("gx", "gy", "gz")


def turns_of(line):
    return -(-max(line - 2, 0) // NEAR) + 1 if line > 1 else 0


def partner_steps(phase, sizes):
    xs = range(1, sizes[0]) if phase else ()
    steps = [(dx, 0, 0) for dx in xs] if phase == 1 else [
        (dx, dy, dz) for dx in tuple(reversed(xs)) + (0,)
        for dy in range(sizes[1]) for dz in range(sizes[2])]
    return [step for step in steps if step != (0, 0, 0)]


def body(
    sizes, cells,
    kry_hbm, schur_hbm, w_hbm, diag_hbm, vel_hbm,
    out, hess,
    schur, w_ref, diag, vel, kry, image, xr, yr, zr, ypack, zpack, xh, yh, zh, yhpack, zhpack, xs, ys, zs,
    rsend, rrecv0, rmid, rrecv1, msend, mrecv0, mmid, mrecv1, lsend, lrecv0, lmid, lrecv1,
    ubuf, abuf, pbuf,
    load_sem, halo_send, halo_recv, sums_sem, line_sem, ready,
):
    place = tuple(lax.axis_index(a) for a in AXES)
    basis = kry_hbm.shape[0]
    bx, by, bz = w_ref.shape
    loads = [
        pltpu.make_async_copy(source, target, load_sem.at[k])
        for k, (source, target) in enumerate((
            (w_hbm, w_ref), (schur_hbm, schur), (kry_hbm, kry.at[0:basis]), (diag_hbm, diag),
            (vel_hbm, vel)))
    ]
    for copy in loads:
        copy.start()
    direct = sizes[0] * sizes[1] * sizes[2] <= DIRECT
    shifted = [[lax.rem(place[d] + k, sizes[d]) for k in range(sizes[d])] for d in range(3)]

    def partners(phase):
        return [tuple(shifted[d][step[d]] for d in range(3))
                for step in partner_steps(phase, sizes)]


    for ref in (xr, yr, zr, xh, yh, zh, xs, ys, zs):
        ref[...] = jnp.zeros_like(ref)

    barrier = pltpu.get_barrier_semaphore()
    line = [
        ((place[0] + step,) + place[1:],
         place[0] < sizes[0] - step if step > 0 else place[0] >= -step)
        for far in range(1, min(NEAR, sizes[0] - 1) + 1) for step in (far, -far)]

    def tell(semaphore, to):
        pl.semaphore_signal(
            semaphore, inc=1, device_id=to, device_id_type=pl.DeviceIdType.MESH)

    for to in partners(0) + ([] if direct else partners(1)):
        tell(barrier, to)
    if direct:
        for to, near in line:
            pl.when(near)(functools.partial(tell, barrier, to))
    turns_needed = turns_of(sizes[0]) if direct else 0

    def pass_on(turn):
        if 0 < turn <= turns_needed:
            for side, (to, near) in enumerate(line if turn < turns_needed else line[:2]):
                pl.when(near)(functools.partial(pl.semaphore_wait, ready.at[turn - 1, side], 1))
        if turn < turns_needed:
            for side, (to, near) in enumerate(line if turn + 1 < turns_needed else line[:2]):
                pl.when(near)(functools.partial(tell, ready.at[turn, side ^ 1], to))


    sent = [[] for _ in range(3)]

    def halo_start(kind, dims, sources, targets):
        for d in dims:
            for side in (0, 1):
                to = list(place)
                to[d] = place[d] + (1 if side == 0 else -1)
                can_send = place[d] < sizes[d] - 1 if side == 0 else place[d] > 0
                source = sources[d][side]
                sent[d].append(math.prod(source.shape))
                pl.when(can_send)(pltpu.make_async_remote_copy(
                    src_ref=source, dst_ref=targets[d][side],
                    send_sem=halo_send.at[d], recv_sem=halo_recv.at[kind, d],
                    device_id=tuple(to), device_id_type=pl.DeviceIdType.MESH).start)

    def landed(ref, semaphore):
        pltpu.make_async_copy(ref, ref, semaphore).wait()

    def halo_wait(kind, targets):
        for d in range(3):
            before, after = place[d] > 0, place[d] < sizes[d] - 1
            semaphore = halo_recv.at[kind, d]
            if sizes[d] > 2:
                pl.when(before & after)(functools.partial(landed, targets[d], semaphore))
                pl.when(before != after)(functools.partial(landed, targets[d].at[0], semaphore))
            elif sizes[d] == 2:
                landed(targets[d].at[0], semaphore)

    def halo_finish():
        for d in range(3):
            before, after = place[d] > 0, place[d] < sizes[d] - 1
            tiles = sum(sent[d]) // 2 // (by * bz)
            if sizes[d] > 2:
                pl.when(before & after)(functools.partial(
                    landed, kry.at[0:tiles, 0:2], halo_send.at[d]))
                pl.when(before != after)(functools.partial(
                    landed, kry.at[0:tiles, 0], halo_send.at[d]))
            elif sizes[d] == 2:
                landed(kry.at[0:tiles, 0], halo_send.at[d])

    def field_targets(kind):
        return tuple(r.at[kind] for r in (xs, ys, zs))

    def field_start(kind, ref):
        halo_start(kind, range(3), ((ref.at[bx - 1], ref.at[0]), (ref, ref), (ref, ref)),
                   tuple((r.at[0], r.at[1]) for r in field_targets(kind)))

    def exchange(send, slots, sem_s, sem_r, phase):
        for at, to in enumerate(partners(phase)):
            pltpu.make_async_remote_copy(
                src_ref=send, dst_ref=slots.at[at], send_sem=sem_s, recv_sem=sem_r,
                device_id=to, device_id_type=pl.DeviceIdType.MESH,
            ).start()
        pending.append(pltpu.make_async_copy(slots, slots, sem_s))
        return pltpu.make_async_copy(slots, slots, sem_r)

    def gather_sum(arrival, own, slots):
        arrival.wait()
        terms = [own] + [slots[k] for k in range(slots.shape[0])]
        while len(terms) > 1:
            terms = [sum(terms[k + 1:k + 2], terms[k]) for k in range(0, len(terms), 2)]
        return terms[0]

    pending = []

    def finish_sends():
        while pending:
            pending.pop().wait()

    groups = (
        (rsend, rrecv0, rmid, rrecv1), (msend, mrecv0, mmid, mrecv1), (lsend, lrecv0, lmid, lrecv1))

    def total_start(k, value):
        send, first = groups[k][:2]
        send[...] = value
        return exchange(send, first, sums_sem.at[2 * k], sums_sem.at[2 * k + 1],
                        2 if direct and k != MIX else 0)

    def total_end(k, value, arrival):
        first, between, second = groups[k][1:]
        value = gather_sum(arrival, value, first)
        if not direct or k == MIX:
            at = 0 if direct else k
            between[...] = value
            arrival = exchange(between, second, line_sem.at[2 * at], line_sem.at[2 * at + 1], 1)
            value = gather_sum(arrival, value, second)
        return value * (1.0 / cells)

    lane3 = lax.broadcasted_iota(jnp.int32, (by, bz), 1)
    row3 = lax.broadcasted_iota(jnp.int32, (by, bz), 0)

    def stencil(v, x_before, x_after, y_before, y_after, z_before, z_after):
        res = []
        for x in range(bx):
            here = v[x]
            xb = v[x - 1] if x > 0 else x_before
            xa = v[x + 1] if x < bx - 1 else x_after
            yb = jnp.where(row3 == 0, y_before[x], pltpu.roll(here, 1, 0))
            ya = jnp.where(row3 == by - 1, y_after[x], pltpu.roll(here, by - 1, 0))
            zb = jnp.where(lane3 == 0, z_before[x], pltpu.roll(here, 1, 1))
            za = jnp.where(lane3 == bz - 1, z_after[x], pltpu.roll(here, bz - 1, 1))
            neighbours = xa + xb + ya + yb + za + zb
            flow = (vel[0, x] * (xa - xb) + vel[1, x] * (ya - yb) + vel[2, x] * (za - zb))
            res.append((6.0 + diag[x]) * here - neighbours + 0.5 * flow)
        return res

    row8 = lax.broadcasted_iota(jnp.int32, (8, LANES), 0)

    def fold(tiles):
        for half in (4, 2, 1):
            low = (row8 & half) == 0
            tiles = [
                jnp.where(low, tiles[k] + pltpu.roll(tiles[k], 8 - half, 0),
                          tiles[k + half] + pltpu.roll(tiles[k + half], half, 0))
                for k in range(half)]
        return tiles[0]

    def dots(v, fields):
        groups = []
        for first in range(0, ROWS, 8):
            tiles = []
            for k in range(first, first + 8):
                field = fields[k] if k < len(fields) else None
                if field is None:
                    tiles.append(None)
                    continue
                total = field(0) * v[0]
                for x in range(1, bx):
                    total = total + field(x) * v[x]
                if by > 8:
                    total = sum(total[8 * t:8 * t + 8] for t in range(1, by // 8)) + total[0:8]
                tiles.append(total)
            if all(tile is None for tile in tiles):
                groups.append(jnp.zeros((8, bz), jnp.float32))
            else:
                groups.append(fold([
                    jnp.zeros((8, bz), jnp.float32) if t is None else t for t in tiles]))
        return jnp.sum(jnp.concatenate(groups, axis=0), axis=1, keepdims=True)

    def of(ref, *at):
        return lambda x: ref[at + (x,)]

    basis_fields = [of(out, i) for i in range(ROWS)]

    loads[0].wait()

    out[KEEP + 1:ROWS] = jnp.zeros((ROWS - KEEP - 1, bx, by, bz), jnp.float32)
    out[KEEP] = w_ref[...]
    deep = kry.shape[0]
    for i in range(basis, deep):
        kry[i] = jnp.zeros((bx, by, bz), jnp.float32)
    loads[1].wait()

    def halves(value):
        high = value.astype(jnp.bfloat16).astype(jnp.float32)
        return high, value - high

    def times(a, b):
        return lax.dot_general(a, b, (((1,), (0,)), ((), ())),
                               precision=lax.Precision.DEFAULT,
                               preferred_element_type=jnp.float32)

    spread = (lax.broadcasted_iota(jnp.int32, (basis, deep * by), 1) // by
              == lax.broadcasted_iota(jnp.int32, (basis, deep * by), 0)).astype(jnp.float32)
    same = (lax.broadcasted_iota(jnp.int32, (by, deep * by), 1) % by
            == lax.broadcasted_iota(jnp.int32, (by, deep * by), 0))
    turns = []
    for part in halves(schur[...]):
        wide = times(part, spread)
        turns.append(jnp.concatenate(
            [jnp.where(same, jnp.broadcast_to(wide[j:j + 1], same.shape), 0.0)
             for j in range(KEEP)], axis=0))
    both = jnp.concatenate(turns, axis=0)
    loads[2].wait()
    for x in range(0, bx, 2):
        pair = range(x, min(x + 2, bx))
        tiles = jnp.concatenate([kry[:, k].reshape(deep * by, bz) for k in pair], axis=1)
        high, low = halves(tiles)
        first = times(both, high)
        found = first[:KEEP * by] + (first[KEEP * by:] + times(turns[0], low))
        for j in range(KEEP):
            for k in pair:
                out[j, k] = found[j * by:(j + 1) * by, (k - x) * bz:(k - x + 1) * bz]

    pl.semaphore_wait(barrier, len(partners(0)) + (
        sum(near.astype(jnp.int32) for _, near in line) if direct else len(partners(1))))
    field_start(0, w_ref)
    pass_on(0)

    def face_start(kind, ref, packs, targets, dims, span):
        (ys_, zs_), (first, last) = packs, span
        halo_start(
            kind, dims,
            ((ref.at[first:last, bx - 1], ref.at[first:last, 0]), (ys_.at[0], ys_.at[1]),
             (zs_.at[0], zs_.at[1])),
            tuple((r.at[0, first:last], r.at[1, first:last]) if d == 0 else (r.at[0], r.at[1])
                  for d, r in enumerate(targets)))

    def pack_faces(ref, packs):
        ys_, zs_ = packs
        for side, (near, edge) in enumerate(((by - 1, bz - 1), (0, 0))):
            for i in range(KEEP):
                ys_[side, i] = ref[i, :, near, :]
            for x in range(bx):
                face = jnp.zeros((by, bz), jnp.float32)
                for i in range(KEEP):
                    face = jnp.where(
                        lane3 == i, pltpu.roll(ref[i, x], (i - edge) % bz, 1), face)
                zs_[side, x] = face

    turned = (3, out, (ypack, zpack), (xr, yr, zr))
    face_start(*turned, (0,), (0, KEEP))
    pack_faces(out, (ypack, zpack))
    face_start(*turned, (1, 2), (0, KEEP))

    row = lax.broadcasted_iota(jnp.int32, (ROWS, LANES), 0)
    lane = lax.broadcasted_iota(jnp.int32, (ROWS, LANES), 1)
    lane1 = lax.broadcasted_iota(jnp.int32, (1, LANES), 1)
    row1 = lax.broadcasted_iota(jnp.int32, (ROWS, 1), 0)

    def as_row(col, shift=0):
        return jnp.sum(jnp.where(row + shift == lane, col, 0.0), axis=0, keepdims=True)

    def as_col(values):
        return jnp.sum(jnp.where(row == lane, values, 0.0), axis=1, keepdims=True)

    gram = jnp.zeros((ROWS, LANES), jnp.float32)
    for j in range(KEEP + 1):
        col = dots([out[j, x] for x in range(bx)],
                   [None] * (j // 8 * 8) + basis_fields[j // 8 * 8:KEEP + 1])
        gram = jnp.where((lane == j) & (row < KEEP + 1), col, gram)
    lane8 = lax.broadcasted_iota(jnp.int32, (8, LANES), 1)
    below = jnp.where(row // 8 > lane // 8, gram, 0.0)
    gram = gram + jnp.concatenate(
        [below, jnp.zeros((LANES - ROWS, LANES), jnp.float32)], axis=0).T[0:ROWS]

    own_sq = jnp.sum(jnp.where((row == KEEP) & (lane == KEEP), gram, 0.0),
                     axis=0, keepdims=True)
    own_sq = jnp.sum(own_sq, axis=1, keepdims=True)
    gram = jnp.where(lane < KEEP, gram, 0.0)
    cut = KEEP + 1
    packed = gram[0:8] + pltpu.roll(gram[8:16], cut, 1) + pltpu.roll(gram[16:24], 2 * cut, 1)
    packed = packed[0:4] + pltpu.roll(packed[4:8], 3 * cut, 1)
    lane4 = lax.broadcasted_iota(jnp.int32, (4, LANES), 1)
    pass_on(1)
    loads[3].wait()
    loads[4].wait()
    halo_wait(0, field_targets(0))
    applied = stencil(
        [w_ref[x] for x in range(bx)], xs[0, 0], xs[0, 1],
        [ys[0, 0, x, by - 1:by, :] for x in range(bx)],
        [ys[0, 1, x, 0:1, :] for x in range(bx)],
        [zs[0, 0, x, :, bz - 1:bz] for x in range(bx)],
        [zs[0, 1, x, :, 0:1] for x in range(bx)],
    )
    for x in range(bx):
        image[0, x] = applied[x]
    field_start(1, image.at[0])
    own = dots(applied, basis_fields[:KEEP + 1] + [None, None, of(image, 0)])
    own = jnp.where(row1 == KEEP + 1, own_sq, own)
    for k in range(6):
        packed = jnp.where(lane4 == cut * (k % 2 * 3 + k // 2) + KEEP,
                           own[4 * k:4 * k + 4], packed)
    for turn in range(2, turns_needed + 1):
        pass_on(turn)
    first_arrival = total_start(0, packed)

    halo_wait(3, (xr, yr, zr))
    applied_faces = (4, ubuf, (yhpack, zhpack), (xh, yh, zh))
    for i in range(KEEP):
        found = stencil(
            [out[i, x] for x in range(bx)], xr[0, i], xr[1, i],
            [yr[0, i, x:x + 1] for x in range(bx)], [yr[1, i, x:x + 1] for x in range(bx)],
            [zr[0, x, :, i:i + 1] for x in range(bx)], [zr[1, x, :, i:i + 1] for x in range(bx)])
        for x in range(bx):
            ubuf[i, x] = found[x]
        if (i + 1) % CHUNK == 0:
            face_start(*applied_faces, (0,), (i + 1 - CHUNK, i + 1))
    pack_faces(ubuf, (yhpack, zhpack))
    face_start(*applied_faces, (1, 2), (0, KEEP))
    ufields = [of(ubuf, i) for i in range(KEEP)]
    def table(fields):
        part = jnp.zeros((ROWS, LANES), jnp.float32)
        for j in range(KEEP):
            part = jnp.where(
                lane == j, dots([ubuf[j, x] for x in range(bx)], fields(j)), part)
        return part

    shares = [table(lambda j: basis_fields[:KEEP] + [of(w_ref), of(image, 0)])]
    halo_wait(1, field_targets(1))
    second = stencil(
        applied, xs[1, 0], xs[1, 1],
        [ys[1, 0, x, by - 1:by, :] for x in range(bx)],
        [ys[1, 1, x, 0:1, :] for x in range(bx)],
        [zs[1, 0, x, :, bz - 1:bz] for x in range(bx)],
        [zs[1, 1, x, :, 0:1] for x in range(bx)],
    )
    for x in range(bx):
        image[1, x] = second[x]
    field_start(2, image.at[1])

    shares.append(table(lambda j: [None] * (j // 8 * 8) + ufields[j // 8 * 8:]))
    mixed = jnp.zeros((8, LANES), jnp.float32)
    for k in range(6):
        part = shares[k // 3][k % 3 * 8:k % 3 * 8 + 8]
        mixed = mixed + (part if k == 0 else pltpu.roll(part, KEEP * k, 1))
    mix_arrival = total_start(1, mixed)
    packed = total_end(0, packed, first_arrival)
    def place_of(at):
        return cut * (at // 4 % 2 * 3 + at // 8)

    again = jnp.concatenate([packed] * (ROWS // 4), axis=0)
    own = jnp.sum(jnp.where(lane == place_of(row) + KEEP, again, 0.0), axis=1, keepdims=True)
    norm_sq = own[KEEP + 1:KEEP + 2]
    image_sq = own[ROWS - 1:ROWS]
    next_row = packed[KEEP % 4:KEEP % 4 + 1]
    next_col = jnp.sum(
        jnp.where((lane == row + place_of(KEEP)) & (row < KEEP), next_row, 0.0),
        axis=1, keepdims=True)
    next_col = next_col + jnp.where(row1 == KEEP, norm_sq, 0.0)
    packed = jnp.concatenate([packed, pltpu.roll(packed, LANES - 3 * cut, 1)], axis=0)
    gram = jnp.concatenate(
        [packed, pltpu.roll(packed, LANES - cut, 1), pltpu.roll(packed, LANES - 2 * cut, 1)],
        axis=0)
    gram = jnp.where((lane < KEEP) & (row <= KEEP), gram, 0.0)
    gram = jnp.where(lane == KEEP, next_col, gram)
    scale = 1.0 / jnp.maximum(jnp.sqrt(norm_sq), 0.5)
    gram = gram * jnp.where(row == KEEP, scale, 1.0) * jnp.where(lane == KEEP, scale, 1.0)
    for x in range(bx):
        out[KEEP, x] = w_ref[x] * scale
    applied = [tile * scale for tile in applied]
    image_sq = image_sq * scale * scale
    own = jnp.where(row1 <= KEEP, own * scale * jnp.where(row1 == KEEP, scale, 1.0), 0.0)

    for x in range(bx):
        abuf[x] = applied[x]
    hcols = []

    def step(count, c_row, c_col, image_sq, gram):
        twice = jnp.where(row == lane, 2.0, 0.0) - gram
        if c_col is None:
            t_col = jnp.sum(twice * c_row, axis=1, keepdims=True)
            t_row = as_row(t_col)
        else:
            t_row = jnp.sum(twice * c_col, axis=0, keepdims=True)
            t_col = as_col(t_row)
        weights = jnp.broadcast_to(t_col, (ROWS, LANES))
        gt_row = jnp.sum(gram * weights, axis=0, keepdims=True)
        length_sq = image_sq + jnp.sum(t_row * (gt_row - 2.0 * c_row), axis=1, keepdims=True)
        length_sq = jnp.maximum(length_sq, 0.0)
        length = jnp.sqrt(length_sq)
        inverse = 1.0 / jnp.maximum(length, 0.5)
        hcols.append(jnp.where(lane1 == count, length, t_row))
        return t_row, t_col, weights, length_sq, inverse

    def less(start, weights, fields):
        for i, field in enumerate(fields):
            weight = jnp.broadcast_to(weights[i:i + 1, :], (by, bz))
            start = [start[x] - weight * field(x) for x in range(bx)]
        return start

    def widen(gram, count, t_row, c_row, length_sq, inverse):
        e_row = t_row - c_row
        e_col = as_col(e_row)
        cross_col = (e_col - jnp.sum(gram * e_row, axis=1, keepdims=True)) * inverse
        cross_row = (e_row - jnp.sum(gram * e_col, axis=0, keepdims=True)) * inverse
        corner = length_sq * inverse * inverse
        gram = jnp.where(row == count, cross_row, jnp.where(lane == count, cross_col, gram))
        return jnp.where((row == count) & (lane == count), corner, gram)

    def pick(values, at):
        return jnp.sum(jnp.where(lane1 == at, values, 0.0), axis=1, keepdims=True)

    count = KEEP + 1
    first_row = as_row(own)
    t_row, t_col, weights, length_sq, inverse = step(count, first_row, own, image_sq, gram)
    newest = [tile * inverse for tile in less(applied, weights, basis_fields[:count])]
    for x in range(bx):
        out[count, x] = newest[x]
    second = [tile * inverse for tile in less(
        [image[1, x] * scale for x in range(bx)], weights, ufields + [of(abuf)])]
    for x in range(bx):
        pbuf[x] = second[x]
    halo_wait(4, (xh, yh, zh))
    halo_wait(2, field_targets(2))
    sides = []
    for side in (0, 1):
        near_row, near_lane = (by - 1, bz - 1) if side == 0 else (0, 0)

        def edge(kind):
            return jnp.concatenate(
                [ys[kind, side, x, near_row:near_row + 1, :] for x in range(bx)], axis=0)

        weight = weights[KEEP:KEEP + 1, :]
        x_part = (xs[2, side] - weight * xs[1, side]) * scale
        y_part = (edge(2) - weight * edge(1)) * scale
        for i in range(KEEP):
            weight = weights[i:i + 1, :]
            x_part = x_part - weight * xh[side, i]
            y_part = y_part - weight * yh[side, i]
        x_part = x_part * inverse
        y_part = y_part * inverse
        z_part = []
        for x in range(bx):
            image_edge, own_edge = (
                zs[kind, side, x, :, near_lane:near_lane + 1] * scale for kind in (2, 1))
            mine = jnp.where(lane3 == KEEP, own_edge, zh[side, x])
            z_part.append(
                (image_edge - jnp.sum(mine * t_row, axis=1, keepdims=True)) * inverse)
        sides.append((x_part, [y_part[x:x + 1] for x in range(bx)], z_part))
    gram = widen(gram, count, t_row, first_row, length_sq, inverse)

    count = KEEP + 2
    grown = ufields + [of(abuf), of(pbuf)]
    p_row = (as_row(dots(second, basis_fields[:count]))
             + as_row(dots(second, grown), 32))
    q_row = as_row(dots(newest, grown[:KEEP + 1]), 32)
    third = stencil(second, sides[0][0], sides[1][0], sides[0][1], sides[1][1],
                    sides[0][2], sides[1][2])
    r_row = (as_row(dots(third, basis_fields[:count]))
             + as_row(dots(third, grown + [lambda x: third[x]]), 32))
    last = jnp.concatenate([p_row, r_row, q_row], axis=0)
    earlier = pending[:]
    pending.clear()
    last_arrival = total_start(2, last)
    for copy in earlier:
        copy.wait()
    halo_finish()
    mixed = total_end(1, mixed, mix_arrival)
    parts = [jnp.where(lane8 < KEEP,
                       mixed if k == 0 else pltpu.roll(mixed, LANES - KEEP * k, 1), 0.0)
             for k in range(6)]
    across = jnp.concatenate(parts[0:3], axis=0)
    inside = jnp.concatenate(parts[3:6], axis=0)
    image_row = across[KEEP + 1:KEEP + 2] * scale
    across = jnp.where(row < KEEP, across, jnp.where(row == KEEP, across * scale, 0.0))
    across = jnp.where((lane == KEEP) & (row <= KEEP), own, across)
    inside = inside * jnp.where(row // 8 > lane // 8, 2.0, 1.0)
    inside = jnp.where(row == KEEP, jnp.where(lane == KEEP, image_sq, 2.0 * image_row), inside)

    last = total_end(2, last, last_arrival)
    shifted_last = pltpu.roll(last, LANES - 32, 1)
    c_row = jnp.where(lane1 < count, last[0:1], 0.0)
    pz_row = jnp.where(lane1 < count, shifted_last[0:1], 0.0)
    rq_row = jnp.where(lane1 < count, last[1:2], 0.0)
    rz_row = jnp.where(lane1 <= count, shifted_last[1:2], 0.0)
    qz_row = jnp.where(lane1 < KEEP + 1, shifted_last[2:3], 0.0)
    across = jnp.where(row == KEEP + 1, qz_row, across)
    across = jnp.where((lane == KEEP + 1) & (row < count), as_col(c_row), across)
    inside = jnp.where(row == KEEP + 1,
                       jnp.where(lane == KEEP + 1, pz_row, 2.0 * pz_row), inside)
    t_row, t_col, weights, length_sq, inverse = step(
        count, c_row, None, pick(pz_row, KEEP + 1), gram)
    gram = widen(gram, count, t_row, c_row, length_sq, inverse)
    h_col = jnp.sum(jnp.where(row == lane, rq_row, 0.0) - across * t_row, axis=1, keepdims=True)
    th = jnp.sum(t_col * h_col, axis=0, keepdims=True)
    corner = jnp.sum(jnp.where(lane1 == KEEP + 1, rz_row, 0.0) - pz_row * t_row,
                     axis=1, keepdims=True)
    corner = (corner - th) * inverse * inverse
    wt_row = jnp.sum(inside * t_col, axis=0, keepdims=True)
    image_sq = jnp.sum(
        jnp.where(lane1 == count, rz_row, (wt_row - 2.0 * rz_row) * t_row),
        axis=1, keepdims=True) * inverse * inverse
    c_col = jnp.where(row1 < count, h_col * inverse, jnp.where(row1 == count, corner, 0.0))
    newest = [tile * inverse for tile in less(second, weights, basis_fields[:count])]
    for x in range(bx):
        out[count, x] = newest[x]
    applied = [tile * inverse for tile in less(third, weights, grown)]
    count = KEEP + 3
    t_row, t_col, weights, length_sq, inverse = step(count, as_row(c_col), c_col, image_sq, gram)
    newest = [tile * inverse for tile in less(applied, weights, basis_fields[:count])]
    for x in range(bx):
        out[count, x] = newest[x]

    for k in range(EXPAND):
        hess[k:k + 1] = hcols[k][:, 0:ROWS]
    finish_sends()


def hand_out(vectors, columns, vectors_hbm, columns_hbm, semaphores):
    copies = [
        pltpu.make_async_copy(source, target, semaphores.at[k])
        for k, (source, target) in enumerate(((vectors, vectors_hbm), (columns, columns_hbm)))]
    for copy in copies:
        copy.start()
    for copy in copies:
        copy.wait()


def per_device(krylov_basis, schur_vectors, next_vector, diag_shift, velocity):
    sizes = tuple(lax.axis_size(a) for a in AXES)
    block = next_vector.shape
    bx, by, bz = block
    cells = float(bx * by * bz * sizes[0] * sizes[1] * sizes[2])
    n0, n1 = sizes[1] * sizes[2], sizes[0]
    nrow = n0 * n1 if n0 * n1 <= DIRECT else n0
    f32 = jnp.float32
    vmem = pl.BlockSpec(memory_space=pltpu.VMEM)
    dma = pltpu.SemaphoreType.DMA
    vectors, columns = pl.pallas_call(
        functools.partial(body, sizes, cells),
        out_shape=(
            pltpu.VMEM((ROWS,) + block, f32),
            pltpu.VMEM((EXPAND, ROWS), f32),
        ),
        in_specs=[
            pl.BlockSpec(memory_space=pl.ANY) for _ in range(5)
        ],
        out_specs=(vmem, vmem),
        scratch_shapes=[
            pltpu.VMEM(schur_vectors.shape[::-1], f32),
            pltpu.VMEM(block, f32),
            pltpu.VMEM(block, f32),
            pltpu.VMEM((3,) + block, f32),
            pltpu.VMEM(((krylov_basis.shape[0] + 15) // 16 * 16,) + block, f32),
            pltpu.VMEM((2,) + block, f32),
            pltpu.VMEM((2, KEEP, by, bz), f32),
            pltpu.VMEM((2, KEEP, bx, bz), f32),
            pltpu.VMEM((2,) + block, f32),
            pltpu.VMEM((2, KEEP, bx, bz), f32),
            pltpu.VMEM((2,) + block, f32),
            pltpu.VMEM((2, KEEP, by, bz), f32),
            pltpu.VMEM((2, KEEP, bx, bz), f32),
            pltpu.VMEM((2,) + block, f32),
            pltpu.VMEM((2, KEEP, bx, bz), f32),
            pltpu.VMEM((2,) + block, f32),
            pltpu.VMEM((EXPAND, 2, by, bz), f32),
            pltpu.VMEM((EXPAND, 2) + block, f32),
            pltpu.VMEM((EXPAND, 2) + block, f32),
            *[pltpu.VMEM(shape, f32) for k, rows in enumerate((4, 8, 3)) for shape in (
                (rows, LANES), ((n0 if k == MIX else nrow) - 1, rows, LANES), (rows, LANES),
                (n1 - 1, rows, LANES))],
            pltpu.VMEM((KEEP,) + block, f32),
            pltpu.VMEM(block, f32),
            pltpu.VMEM(block, f32),
            dma((5,)), dma((3,)), dma((5, 3)),
            dma((6,)), dma((2 if nrow > n0 else 6,)),
            pltpu.SemaphoreType.REGULAR((max(turns_of(sizes[0]), 1), 2 * NEAR)),
        ],
        compiler_params=pltpu.CompilerParams(collective_id=0, has_side_effects=True),
    )(krylov_basis, schur_vectors.T, next_vector, diag_shift, velocity)
    results = [pltpu.with_memory_space_constraint(r, pltpu.VMEM) for r in (vectors, columns)]
    vectors, columns = pl.pallas_call(
        hand_out,
        out_shape=[jax.ShapeDtypeStruct(r.shape, f32) for r in results],
        in_specs=[vmem, vmem],
        out_specs=[pl.BlockSpec(memory_space=pl.ANY)] * 2,
        scratch_shapes=[dma((2,))],
    )(*results)
    return vectors, columns.T


def solution(mesh):
    in_specs = (
        P(None, "gx", "gy", "gz"),
        P(),
        P("gx", "gy", "gz"),
        P("gx", "gy", "gz"),
        P(None, "gx", "gy", "gz"),
    )
    out_specs = (P(None, "gx", "gy", "gz"), P())
    return jax.shard_map(
        per_device, mesh=mesh, in_specs=in_specs, out_specs=out_specs, check_vma=False
    )
```

```python
import functools
import math

import jax
import jax.numpy as jnp
from jax import lax
from jax.experimental import pallas as pl
from jax.experimental.pallas import tpu as pltpu
from jax.sharding import PartitionSpec as P

KEEP = 20
EXPAND = 3
ROWS = 24
LANES = 128
DIRECT = 64
CHUNK = 5
MIX = 1
NEAR = 2
SLOT = (0, 1, 0, 2, 3)
AXES = ("gx", "gy", "gz")


def turns_of(line):
    return -(-max(line - 2, 0) // NEAR) + 1 if line > 1 else 0


def partner_steps(phase, sizes):
    xs = range(1, sizes[0]) if phase else ()
    steps = [(dx, 0, 0) for dx in xs] if phase == 1 else [
        (dx, dy, dz) for dx in tuple(reversed(xs)) + (0,)
        for dy in range(sizes[1]) for dz in range(sizes[2])]
    return [step for step in steps if step != (0, 0, 0)]


def body(
    sizes, cells,
    kry_hbm, schur_hbm, w_hbm, diag_hbm, vel_hbm,
    out, hess,
    schur, w_ref, diag, vel, kry, image, xr, yr, zr, ypack, zpack, xh, yh, zh, yhpack, zhpack, xs, ys, zs,
    rsend, rrecv0, rmid, rrecv1, msend, mrecv0, mmid, mrecv1, lsend, lrecv0, lmid, lrecv1,
    ubuf, abuf, pbuf,
    load_sem, halo_send, halo_recv, sums_sem, line_sem, ready,
):
    place = tuple(lax.axis_index(a) for a in AXES)
    basis = kry_hbm.shape[0]
    bx, by, bz = w_ref.shape
    loads = [
        pltpu.make_async_copy(source, target, load_sem.at[k])
        for k, (source, target) in enumerate((
            (w_hbm, w_ref), (schur_hbm, schur), (kry_hbm, kry.at[0:basis]), (diag_hbm, diag),
            (vel_hbm, vel)))
    ]
    for copy in loads:
        copy.start()
    direct = sizes[0] * sizes[1] * sizes[2] <= DIRECT
    shifted = [[lax.rem(place[d] + k, sizes[d]) for k in range(sizes[d])] for d in range(3)]

    def partners(phase):
        return [tuple(shifted[d][step[d]] for d in range(3))
                for step in partner_steps(phase, sizes)]


    for ref in (xr, yr, zr, xh, yh, zh, xs, ys, zs):
        ref[...] = jnp.zeros_like(ref)

    barrier = pltpu.get_barrier_semaphore()
    line = [
        ((place[0] + step,) + place[1:],
         place[0] < sizes[0] - step if step > 0 else place[0] >= -step)
        for far in range(1, min(NEAR, sizes[0] - 1) + 1) for step in (far, -far)]

    def tell(semaphore, to):
        pl.semaphore_signal(
            semaphore, inc=1, device_id=to, device_id_type=pl.DeviceIdType.MESH)

    for to in partners(0) + ([] if direct else partners(1)):
        tell(barrier, to)
    if direct:
        for to, near in line:
            pl.when(near)(functools.partial(tell, barrier, to))
    turns_needed = turns_of(sizes[0]) if direct else 0

    def pass_on(turn):
        if 0 < turn <= turns_needed:
            for side, (to, near) in enumerate(line if turn < turns_needed else line[:2]):
                pl.when(near)(functools.partial(pl.semaphore_wait, ready.at[2 * NEAR * (turn - 1) + side], 1))
        if turn < turns_needed:
            for side, (to, near) in enumerate(line if turn + 1 < turns_needed else line[:2]):
                pl.when(near)(functools.partial(tell, ready.at[2 * NEAR * turn + (side ^ 1)], to))


    sent = [[] for _ in range(3)]

    def halo_start(kind, dims, sources, targets):
        for d in dims:
            for side in (0, 1):
                to = list(place)
                to[d] = place[d] + (1 if side == 0 else -1)
                can_send = place[d] < sizes[d] - 1 if side == 0 else place[d] > 0
                source = sources[d][side]
                sent[d].append(math.prod(source.shape))
                pl.when(can_send)(pltpu.make_async_remote_copy(
                    src_ref=source, dst_ref=targets[d][side],
                    send_sem=halo_send.at[d], recv_sem=halo_recv.at[SLOT[kind], d],
                    device_id=tuple(to), device_id_type=pl.DeviceIdType.MESH).start)

    def landed(ref, semaphore):
        pltpu.make_async_copy(ref, ref, semaphore).wait()

    def halo_wait(kind, targets):
        for d in range(3):
            before, after = place[d] > 0, place[d] < sizes[d] - 1
            semaphore = halo_recv.at[SLOT[kind], d]
            if sizes[d] > 2:
                pl.when(before & after)(functools.partial(landed, targets[d], semaphore))
                pl.when(before != after)(functools.partial(landed, targets[d].at[0], semaphore))
            elif sizes[d] == 2:
                landed(targets[d].at[0], semaphore)

    def halo_finish():
        for d in range(3):
            before, after = place[d] > 0, place[d] < sizes[d] - 1
            tiles = sum(sent[d]) // 2 // (by * bz)
            if sizes[d] > 2:
                pl.when(before & after)(functools.partial(
                    landed, kry.at[0:tiles, 0:2], halo_send.at[d]))
                pl.when(before != after)(functools.partial(
                    landed, kry.at[0:tiles, 0], halo_send.at[d]))
            elif sizes[d] == 2:
                landed(kry.at[0:tiles, 0], halo_send.at[d])

    def field_targets(kind):
        return tuple(r.at[kind] for r in (xs, ys, zs))

    def field_start(kind, ref):
        halo_start(kind, range(3), ((ref.at[bx - 1], ref.at[0]), (ref, ref), (ref, ref)),
                   tuple((r.at[0], r.at[1]) for r in field_targets(kind)))

    def exchange(send, slots, sem_s, sem_r, phase):
        for at, to in enumerate(partners(phase)):
            pltpu.make_async_remote_copy(
                src_ref=send, dst_ref=slots.at[at], send_sem=sem_s, recv_sem=sem_r,
                device_id=to, device_id_type=pl.DeviceIdType.MESH,
            ).start()
        pending.append(pltpu.make_async_copy(slots, slots, sem_s))
        return pltpu.make_async_copy(slots, slots, sem_r)

    def gather_sum(arrival, own, slots):
        arrival.wait()
        terms = [own] + [slots[k] for k in range(slots.shape[0])]
        while len(terms) > 1:
            terms = [sum(terms[k + 1:k + 2], terms[k]) for k in range(0, len(terms), 2)]
        return terms[0]

    pending = []

    def finish_sends():
        while pending:
            pending.pop().wait()

    groups = (
        (rsend, rrecv0, rmid, rrecv1), (msend, mrecv0, mmid, mrecv1), (lsend, lrecv0, lmid, lrecv1))

    def total_start(k, value):
        send, first = groups[k][:2]
        send[...] = value
        return exchange(send, first, sums_sem.at[2 * k], sums_sem.at[2 * k + 1],
                        2 if direct and k != MIX else 0)

    def total_end(k, value, arrival):
        first, between, second = groups[k][1:]
        value = gather_sum(arrival, value, first)
        if not direct or k == MIX:
            at = 0 if direct else k
            between[...] = value
            arrival = exchange(between, second, line_sem.at[2 * at], line_sem.at[2 * at + 1], 1)
            value = gather_sum(arrival, value, second)
        return value * (1.0 / cells)

    lane3 = lax.broadcasted_iota(jnp.int32, (by, bz), 1)
    row3 = lax.broadcasted_iota(jnp.int32, (by, bz), 0)

    def stencil(v, x_before, x_after, y_before, y_after, z_before, z_after):
        res = []
        for x in range(bx):
            here = v[x]
            xb = v[x - 1] if x > 0 else x_before
            xa = v[x + 1] if x < bx - 1 else x_after
            yb = jnp.where(row3 == 0, y_before[x], pltpu.roll(here, 1, 0))
            ya = jnp.where(row3 == by - 1, y_after[x], pltpu.roll(here, by - 1, 0))
            zb = jnp.where(lane3 == 0, z_before[x], pltpu.roll(here, 1, 1))
            za = jnp.where(lane3 == bz - 1, z_after[x], pltpu.roll(here, bz - 1, 1))
            neighbours = xa + xb + ya + yb + za + zb
            flow = (vel[0, x] * (xa - xb) + vel[1, x] * (ya - yb) + vel[2, x] * (za - zb))
            res.append((6.0 + diag[x]) * here - neighbours + 0.5 * flow)
        return res

    row8 = lax.broadcasted_iota(jnp.int32, (8, LANES), 0)

    def fold(tiles):
        for half in (4, 2, 1):
            low = (row8 & half) == 0
            tiles = [
                jnp.where(low, tiles[k] + pltpu.roll(tiles[k], 8 - half, 0),
                          tiles[k + half] + pltpu.roll(tiles[k + half], half, 0))
                for k in range(half)]
        return tiles[0]

    def dots(v, fields):
        groups = []
        for first in range(0, ROWS, 8):
            tiles = []
            for k in range(first, first + 8):
                field = fields[k] if k < len(fields) else None
                if field is None:
                    tiles.append(None)
                    continue
                total = field(0) * v[0]
                for x in range(1, bx):
                    total = total + field(x) * v[x]
                if by > 8:
                    total = sum(total[8 * t:8 * t + 8] for t in range(1, by // 8)) + total[0:8]
                tiles.append(total)
            if all(tile is None for tile in tiles):
                groups.append(jnp.zeros((8, bz), jnp.float32))
            else:
                groups.append(fold([
                    jnp.zeros((8, bz), jnp.float32) if t is None else t for t in tiles]))
        return jnp.sum(jnp.concatenate(groups, axis=0), axis=1, keepdims=True)

    def of(ref, *at):
        return lambda x: ref[at + (x,)]

    basis_fields = [of(out, i) for i in range(ROWS)]

    loads[0].wait()

    out[KEEP + 1:ROWS] = jnp.zeros((ROWS - KEEP - 1, bx, by, bz), jnp.float32)
    out[KEEP] = w_ref[...]
    deep = kry.shape[0]
    for i in range(basis, deep):
        kry[i] = jnp.zeros((bx, by, bz), jnp.float32)
    loads[1].wait()

    def halves(value):
        high = value.astype(jnp.bfloat16).astype(jnp.float32)
        return high, value - high

    def times(a, b):
        return lax.dot_general(a, b, (((1,), (0,)), ((), ())),
                               precision=lax.Precision.DEFAULT,
                               preferred_element_type=jnp.float32)

    spread = (lax.broadcasted_iota(jnp.int32, (basis, deep * by), 1) // by
              == lax.broadcasted_iota(jnp.int32, (basis, deep * by), 0)).astype(jnp.float32)
    same = (lax.broadcasted_iota(jnp.int32, (by, deep * by), 1) % by
            == lax.broadcasted_iota(jnp.int32, (by, deep * by), 0))
    turns = []
    for part in halves(schur[...]):
        wide = times(part, spread)
        turns.append(jnp.concatenate(
            [jnp.where(same, jnp.broadcast_to(wide[j:j + 1], same.shape), 0.0)
             for j in range(KEEP)], axis=0))
    both = jnp.concatenate(turns, axis=0)
    loads[2].wait()
    for x in range(0, bx, 2):
        pair = range(x, min(x + 2, bx))
        tiles = jnp.concatenate([kry[:, k].reshape(deep * by, bz) for k in pair], axis=1)
        high, low = halves(tiles)
        first = times(both, high)
        found = first[:KEEP * by] + (first[KEEP * by:] + times(turns[0], low))
        for j in range(KEEP):
            for k in pair:
                out[j, k] = found[j * by:(j + 1) * by, (k - x) * bz:(k - x + 1) * bz]

    pl.semaphore_wait(barrier, len(partners(0)) + (
        sum(near.astype(jnp.int32) for _, near in line) if direct else len(partners(1))))
    field_start(0, w_ref)
    pass_on(0)

    def face_start(kind, ref, packs, targets, dims, span):
        (ys_, zs_), (first, last) = packs, span
        halo_start(
            kind, dims,
            ((ref.at[first:last, bx - 1], ref.at[first:last, 0]), (ys_.at[0], ys_.at[1]),
             (zs_.at[0], zs_.at[1])),
            tuple((r.at[0, first:last], r.at[1, first:last]) if d == 0 else (r.at[0], r.at[1])
                  for d, r in enumerate(targets)))

    def pack_faces(ref, packs):
        ys_, zs_ = packs
        for side, (near, edge) in enumerate(((by - 1, bz - 1), (0, 0))):
            for i in range(KEEP):
                ys_[side, i] = ref[i, :, near, :]
            for x in range(bx):
                face = jnp.zeros((by, bz), jnp.float32)
                for i in range(KEEP):
                    face = jnp.where(
                        lane3 == i, pltpu.roll(ref[i, x], (i - edge) % bz, 1), face)
                zs_[side, x] = face

    turned = (3, out, (ypack, zpack), (xr, yr, zr))
    face_start(*turned, (0,), (0, KEEP))
    pack_faces(out, (ypack, zpack))
    face_start(*turned, (1, 2), (0, KEEP))

    row = lax.broadcasted_iota(jnp.int32, (ROWS, LANES), 0)
    lane = lax.broadcasted_iota(jnp.int32, (ROWS, LANES), 1)
    lane1 = lax.broadcasted_iota(jnp.int32, (1, LANES), 1)
    row1 = lax.broadcasted_iota(jnp.int32, (ROWS, 1), 0)

    def as_row(col, shift=0):
        return jnp.sum(jnp.where(row + shift == lane, col, 0.0), axis=0, keepdims=True)

    def as_col(values):
        return jnp.sum(jnp.where(row == lane, values, 0.0), axis=1, keepdims=True)

    gram = jnp.zeros((ROWS, LANES), jnp.float32)
    for j in range(KEEP + 1):
        col = dots([out[j, x] for x in range(bx)],
                   [None] * (j // 8 * 8) + basis_fields[j // 8 * 8:KEEP + 1])
        gram = jnp.where((lane == j) & (row < KEEP + 1), col, gram)
    lane8 = lax.broadcasted_iota(jnp.int32, (8, LANES), 1)
    below = jnp.where(row // 8 > lane // 8, gram, 0.0)
    gram = gram + jnp.concatenate(
        [below, jnp.zeros((LANES - ROWS, LANES), jnp.float32)], axis=0).T[0:ROWS]

    own_sq = jnp.sum(jnp.where((row == KEEP) & (lane == KEEP), gram, 0.0),
                     axis=0, keepdims=True)
    own_sq = jnp.sum(own_sq, axis=1, keepdims=True)
    gram = jnp.where(lane < KEEP, gram, 0.0)
    cut = KEEP + 1
    packed = gram[0:8] + pltpu.roll(gram[8:16], cut, 1) + pltpu.roll(gram[16:24], 2 * cut, 1)
    packed = packed[0:4] + pltpu.roll(packed[4:8], 3 * cut, 1)
    lane4 = lax.broadcasted_iota(jnp.int32, (4, LANES), 1)
    pass_on(1)
    loads[3].wait()
    loads[4].wait()
    halo_wait(0, field_targets(0))
    applied = stencil(
        [w_ref[x] for x in range(bx)], xs[0, 0], xs[0, 1],
        [ys[0, 0, x, by - 1:by, :] for x in range(bx)],
        [ys[0, 1, x, 0:1, :] for x in range(bx)],
        [zs[0, 0, x, :, bz - 1:bz] for x in range(bx)],
        [zs[0, 1, x, :, 0:1] for x in range(bx)],
    )
    for x in range(bx):
        image[0, x] = applied[x]
    field_start(1, image.at[0])
    own = dots(applied, basis_fields[:KEEP + 1] + [None, None, of(image, 0)])
    own = jnp.where(row1 == KEEP + 1, own_sq, own)
    for k in range(6):
        packed = jnp.where(lane4 == cut * (k % 2 * 3 + k // 2) + KEEP,
                           own[4 * k:4 * k + 4], packed)
    for turn in range(2, turns_needed + 1):
        pass_on(turn)
    first_arrival = total_start(0, packed)

    halo_wait(3, (xr, yr, zr))
    applied_faces = (4, ubuf, (yhpack, zhpack), (xh, yh, zh))
    for i in range(KEEP):
        found = stencil(
            [out[i, x] for x in range(bx)], xr[0, i], xr[1, i],
            [yr[0, i, x:x + 1] for x in range(bx)], [yr[1, i, x:x + 1] for x in range(bx)],
            [zr[0, x, :, i:i + 1] for x in range(bx)], [zr[1, x, :, i:i + 1] for x in range(bx)])
        for x in range(bx):
            ubuf[i, x] = found[x]
        if (i + 1) % CHUNK == 0:
            face_start(*applied_faces, (0,), (i + 1 - CHUNK, i + 1))
    pack_faces(ubuf, (yhpack, zhpack))
    face_start(*applied_faces, (1, 2), (0, KEEP))
    ufields = [of(ubuf, i) for i in range(KEEP)]
    def table(fields):
        part = jnp.zeros((ROWS, LANES), jnp.float32)
        for j in range(KEEP):
            part = jnp.where(
                lane == j, dots([ubuf[j, x] for x in range(bx)], fields(j)), part)
        return part

    shares = [table(lambda j: basis_fields[:KEEP] + [of(w_ref), of(image, 0)])]
    halo_wait(1, field_targets(1))
    second = stencil(
        applied, xs[1, 0], xs[1, 1],
        [ys[1, 0, x, by - 1:by, :] for x in range(bx)],
        [ys[1, 1, x, 0:1, :] for x in range(bx)],
        [zs[1, 0, x, :, bz - 1:bz] for x in range(bx)],
        [zs[1, 1, x, :, 0:1] for x in range(bx)],
    )
    for x in range(bx):
        image[1, x] = second[x]
    field_start(2, image.at[1])

    shares.append(table(lambda j: [None] * (j // 8 * 8) + ufields[j // 8 * 8:]))
    mixed = jnp.zeros((8, LANES), jnp.float32)
    for k in range(6):
        part = shares[k // 3][k % 3 * 8:k % 3 * 8 + 8]
        mixed = mixed + (part if k == 0 else pltpu.roll(part, KEEP * k, 1))
    mix_arrival = total_start(1, mixed)
    packed = total_end(0, packed, first_arrival)
    def place_of(at):
        return cut * (at // 4 % 2 * 3 + at // 8)

    again = jnp.concatenate([packed] * (ROWS // 4), axis=0)
    own = jnp.sum(jnp.where(lane == place_of(row) + KEEP, again, 0.0), axis=1, keepdims=True)
    norm_sq = own[KEEP + 1:KEEP + 2]
    image_sq = own[ROWS - 1:ROWS]
    next_row = packed[KEEP % 4:KEEP % 4 + 1]
    next_col = jnp.sum(
        jnp.where((lane == row + place_of(KEEP)) & (row < KEEP), next_row, 0.0),
        axis=1, keepdims=True)
    next_col = next_col + jnp.where(row1 == KEEP, norm_sq, 0.0)
    packed = jnp.concatenate([packed, pltpu.roll(packed, LANES - 3 * cut, 1)], axis=0)
    gram = jnp.concatenate(
        [packed, pltpu.roll(packed, LANES - cut, 1), pltpu.roll(packed, LANES - 2 * cut, 1)],
        axis=0)
    gram = jnp.where((lane < KEEP) & (row <= KEEP), gram, 0.0)
    gram = jnp.where(lane == KEEP, next_col, gram)
    scale = 1.0 / jnp.maximum(jnp.sqrt(norm_sq), 0.5)
    gram = gram * jnp.where(row == KEEP, scale, 1.0) * jnp.where(lane == KEEP, scale, 1.0)
    for x in range(bx):
        out[KEEP, x] = w_ref[x] * scale
    applied = [tile * scale for tile in applied]
    image_sq = image_sq * scale * scale
    own = jnp.where(row1 <= KEEP, own * scale * jnp.where(row1 == KEEP, scale, 1.0), 0.0)

    for x in range(bx):
        abuf[x] = applied[x]
    hcols = []

    def step(count, c_row, c_col, image_sq, gram):
        twice = jnp.where(row == lane, 2.0, 0.0) - gram
        if c_col is None:
            t_col = jnp.sum(twice * c_row, axis=1, keepdims=True)
            t_row = as_row(t_col)
        else:
            t_row = jnp.sum(twice * c_col, axis=0, keepdims=True)
            t_col = as_col(t_row)
        weights = jnp.broadcast_to(t_col, (ROWS, LANES))
        gt_row = jnp.sum(gram * weights, axis=0, keepdims=True)
        length_sq = image_sq + jnp.sum(t_row * (gt_row - 2.0 * c_row), axis=1, keepdims=True)
        length_sq = jnp.maximum(length_sq, 0.0)
        length = jnp.sqrt(length_sq)
        inverse = 1.0 / jnp.maximum(length, 0.5)
        hcols.append(jnp.where(lane1 == count, length, t_row))
        return t_row, t_col, weights, length_sq, inverse

    def less(start, weights, fields):
        for i, field in enumerate(fields):
            weight = jnp.broadcast_to(weights[i:i + 1, :], (by, bz))
            start = [start[x] - weight * field(x) for x in range(bx)]
        return start

    def widen(gram, count, t_row, c_row, length_sq, inverse):
        e_row = t_row - c_row
        e_col = as_col(e_row)
        cross_col = (e_col - jnp.sum(gram * e_row, axis=1, keepdims=True)) * inverse
        cross_row = (e_row - jnp.sum(gram * e_col, axis=0, keepdims=True)) * inverse
        corner = length_sq * inverse * inverse
        gram = jnp.where(row == count, cross_row, jnp.where(lane == count, cross_col, gram))
        return jnp.where((row == count) & (lane == count), corner, gram)

    def pick(values, at):
        return jnp.sum(jnp.where(lane1 == at, values, 0.0), axis=1, keepdims=True)

    count = KEEP + 1
    first_row = as_row(own)
    t_row, t_col, weights, length_sq, inverse = step(count, first_row, own, image_sq, gram)
    newest = [tile * inverse for tile in less(applied, weights, basis_fields[:count])]
    for x in range(bx):
        out[count, x] = newest[x]
    second = [tile * inverse for tile in less(
        [image[1, x] * scale for x in range(bx)], weights, ufields + [of(abuf)])]
    for x in range(bx):
        pbuf[x] = second[x]
    halo_wait(4, (xh, yh, zh))
    halo_wait(2, field_targets(2))
    sides = []
    for side in (0, 1):
        near_row, near_lane = (by - 1, bz - 1) if side == 0 else (0, 0)

        def edge(kind):
            return jnp.concatenate(
                [ys[kind, side, x, near_row:near_row + 1, :] for x in range(bx)], axis=0)

        weight = weights[KEEP:KEEP + 1, :]
        x_part = (xs[2, side] - weight * xs[1, side]) * scale
        y_part = (edge(2) - weight * edge(1)) * scale
        for i in range(KEEP):
            weight = weights[i:i + 1, :]
            x_part = x_part - weight * xh[side, i]
            y_part = y_part - weight * yh[side, i]
        x_part = x_part * inverse
        y_part = y_part * inverse
        z_part = []
        for x in range(bx):
            image_edge, own_edge = (
                zs[kind, side, x, :, near_lane:near_lane + 1] * scale for kind in (2, 1))
            mine = jnp.where(lane3 == KEEP, own_edge, zh[side, x])
            z_part.append(
                (image_edge - jnp.sum(mine * t_row, axis=1, keepdims=True)) * inverse)
        sides.append((x_part, [y_part[x:x + 1] for x in range(bx)], z_part))
    gram = widen(gram, count, t_row, first_row, length_sq, inverse)

    count = KEEP + 2
    grown = ufields + [of(abuf), of(pbuf)]
    p_row = (as_row(dots(second, basis_fields[:count]))
             + as_row(dots(second, grown), 32))
    q_row = as_row(dots(newest, grown[:KEEP + 1]), 32)
    third = stencil(second, sides[0][0], sides[1][0], sides[0][1], sides[1][1],
                    sides[0][2], sides[1][2])
    r_row = (as_row(dots(third, basis_fields[:count]))
             + as_row(dots(third, grown + [lambda x: third[x]]), 32))
    last = jnp.concatenate([p_row, r_row, q_row], axis=0)
    earlier = pending[:]
    pending.clear()
    last_arrival = total_start(2, last)
    for copy in earlier:
        copy.wait()
    halo_finish()
    mixed = total_end(1, mixed, mix_arrival)
    parts = [jnp.where(lane8 < KEEP,
                       mixed if k == 0 else pltpu.roll(mixed, LANES - KEEP * k, 1), 0.0)
             for k in range(6)]
    across = jnp.concatenate(parts[0:3], axis=0)
    inside = jnp.concatenate(parts[3:6], axis=0)
    image_row = across[KEEP + 1:KEEP + 2] * scale
    across = jnp.where(row < KEEP, across, jnp.where(row == KEEP, across * scale, 0.0))
    across = jnp.where((lane == KEEP) & (row <= KEEP), own, across)
    inside = inside * jnp.where(row // 8 > lane // 8, 2.0, 1.0)
    inside = jnp.where(row == KEEP, jnp.where(lane == KEEP, image_sq, 2.0 * image_row), inside)

    last = total_end(2, last, last_arrival)
    shifted_last = pltpu.roll(last, LANES - 32, 1)
    c_row = jnp.where(lane1 < count, last[0:1], 0.0)
    pz_row = jnp.where(lane1 < count, shifted_last[0:1], 0.0)
    rq_row = jnp.where(lane1 < count, last[1:2], 0.0)
    rz_row = jnp.where(lane1 <= count, shifted_last[1:2], 0.0)
    qz_row = jnp.where(lane1 < KEEP + 1, shifted_last[2:3], 0.0)
    across = jnp.where(row == KEEP + 1, qz_row, across)
    across = jnp.where((lane == KEEP + 1) & (row < count), as_col(c_row), across)
    inside = jnp.where(row == KEEP + 1,
                       jnp.where(lane == KEEP + 1, pz_row, 2.0 * pz_row), inside)
    t_row, t_col, weights, length_sq, inverse = step(
        count, c_row, None, pick(pz_row, KEEP + 1), gram)
    gram = widen(gram, count, t_row, c_row, length_sq, inverse)
    h_col = jnp.sum(jnp.where(row == lane, rq_row, 0.0) - across * t_row, axis=1, keepdims=True)
    th = jnp.sum(t_col * h_col, axis=0, keepdims=True)
    corner = jnp.sum(jnp.where(lane1 == KEEP + 1, rz_row, 0.0) - pz_row * t_row,
                     axis=1, keepdims=True)
    corner = (corner - th) * inverse * inverse
    wt_row = jnp.sum(inside * t_col, axis=0, keepdims=True)
    image_sq = jnp.sum(
        jnp.where(lane1 == count, rz_row, (wt_row - 2.0 * rz_row) * t_row),
        axis=1, keepdims=True) * inverse * inverse
    c_col = jnp.where(row1 < count, h_col * inverse, jnp.where(row1 == count, corner, 0.0))
    newest = [tile * inverse for tile in less(second, weights, basis_fields[:count])]
    for x in range(bx):
        out[count, x] = newest[x]
    applied = [tile * inverse for tile in less(third, weights, grown)]
    count = KEEP + 3
    t_row, t_col, weights, length_sq, inverse = step(count, as_row(c_col), c_col, image_sq, gram)
    newest = [tile * inverse for tile in less(applied, weights, basis_fields[:count])]
    for x in range(bx):
        out[count, x] = newest[x]

    for k in range(EXPAND):
        hess[k:k + 1] = hcols[k][:, 0:ROWS]
    finish_sends()


def hand_out(vectors, columns, vectors_hbm, columns_hbm, semaphores):
    copies = [
        pltpu.make_async_copy(source, target, semaphores.at[k])
        for k, (source, target) in enumerate(((vectors, vectors_hbm), (columns, columns_hbm)))]
    for copy in copies:
        copy.start()
    for copy in copies:
        copy.wait()


def per_device(krylov_basis, schur_vectors, next_vector, diag_shift, velocity):
    sizes = tuple(lax.axis_size(a) for a in AXES)
    block = next_vector.shape
    bx, by, bz = block
    cells = float(bx * by * bz * sizes[0] * sizes[1] * sizes[2])
    n0, n1 = sizes[1] * sizes[2], sizes[0]
    nrow = n0 * n1 if n0 * n1 <= DIRECT else n0
    f32 = jnp.float32
    vmem = pl.BlockSpec(memory_space=pltpu.VMEM)
    dma = pltpu.SemaphoreType.DMA
    vectors, columns = pl.pallas_call(
        functools.partial(body, sizes, cells),
        out_shape=(
            pltpu.VMEM((ROWS,) + block, f32),
            pltpu.VMEM((EXPAND, ROWS), f32),
        ),
        in_specs=[
            pl.BlockSpec(memory_space=pl.ANY) for _ in range(5)
        ],
        out_specs=(vmem, vmem),
        scratch_shapes=[
            pltpu.VMEM(schur_vectors.shape[::-1], f32),
            pltpu.VMEM(block, f32),
            pltpu.VMEM(block, f32),
            pltpu.VMEM((3,) + block, f32),
            pltpu.VMEM(((krylov_basis.shape[0] + 15) // 16 * 16,) + block, f32),
            pltpu.VMEM((2,) + block, f32),
            pltpu.VMEM((2, KEEP, by, bz), f32),
            pltpu.VMEM((2, KEEP, bx, bz), f32),
            pltpu.VMEM((2,) + block, f32),
            pltpu.VMEM((2, KEEP, bx, bz), f32),
            pltpu.VMEM((2,) + block, f32),
            pltpu.VMEM((2, KEEP, by, bz), f32),
            pltpu.VMEM((2, KEEP, bx, bz), f32),
            pltpu.VMEM((2,) + block, f32),
            pltpu.VMEM((2, KEEP, bx, bz), f32),
            pltpu.VMEM((2,) + block, f32),
            pltpu.VMEM((EXPAND, 2, by, bz), f32),
            pltpu.VMEM((EXPAND, 2) + block, f32),
            pltpu.VMEM((EXPAND, 2) + block, f32),
            *[pltpu.VMEM(shape, f32) for k, rows in enumerate((4, 8, 3)) for shape in (
                (rows, LANES), ((n0 if k == MIX else nrow) - 1, rows, LANES), (rows, LANES),
                (n1 - 1, rows, LANES))],
            pltpu.VMEM((KEEP,) + block, f32),
            pltpu.VMEM(block, f32),
            pltpu.VMEM(block, f32),
            dma((5,)), dma((3,)), dma((4, 3)),
            dma((6,)), dma((2 if nrow > n0 else 6,)),
            pltpu.SemaphoreType.REGULAR((2 * NEAR * max(turns_of(sizes[0]) - 1, 0) + 2,)),
        ],
        compiler_params=pltpu.CompilerParams(collective_id=0, has_side_effects=True),
    )(krylov_basis, schur_vectors.T, next_vector, diag_shift, velocity)
    results = [pltpu.with_memory_space_constraint(r, pltpu.VMEM) for r in (vectors, columns)]
    vectors, columns = pl.pallas_call(
        hand_out,
        out_shape=[jax.ShapeDtypeStruct(r.shape, f32) for r in results],
        in_specs=[vmem, vmem],
        out_specs=[pl.BlockSpec(memory_space=pl.ANY)] * 2,
        scratch_shapes=[dma((2,))],
    )(*results)
    return vectors, columns.T


def solution(mesh):
    in_specs = (
        P(None, "gx", "gy", "gz"),
        P(),
        P("gx", "gy", "gz"),
        P("gx", "gy", "gz"),
        P(None, "gx", "gy", "gz"),
    )
    out_specs = (P(None, "gx", "gy", "gz"), P())
    return jax.shard_map(
        per_device, mesh=mesh, in_specs=in_specs, out_specs=out_specs, check_vma=False
    )
```
